32 devices in a mesh: tile: 2 (over y), beam: 4 (over z), bl: 2 (over x), pol: 2 (over core).
Axes of the slice: x: 2, y: 2, z: 4, core: 2. Of those that a mesh axis runs over, the one named last changes fastest.
Arguments:
- sky_model: bfloat16 [4096, 4096], P(('tile', 'bl', 'pol'), 'beam'), parts along dimension 0, may hold values from -6 to 6
- beam_pattern: bfloat16 [8, 2048, 2048], P(('tile', 'beam'), ('bl', 'pol')), parts along dimension 0, may hold values from 0.099609375 to 1
- kernels: bfloat16 [8, 256, 128, 128], P(('tile', 'beam'), ('bl', 'pol')), parts along dimension 0, may hold values from -0.5 to 0.5
- observed: float32 [8, 256, 2, 128], P(('tile', 'beam'), ('bl', 'pol')), parts along dimension 0, may hold values from -6 to 6
- tile_owner: int32 [8, 256, 1], P(('tile', 'beam'), ('bl', 'pol')), parts along dimension 0, may hold values from 0 to 3; in each aligned block of 64 rows (0 to 63, 64 to 127, ..., all dimensions but the last counted through in order) at most 32 rows name the same one
- tile_local: int32 [8, 256], P(('tile', 'beam'), ('bl', 'pol')), parts along dimension 0, may hold values from 0 to 4095
- vis_count: int32 [8, 256], P(('tile', 'beam'), ('bl', 'pol')), parts along dimension 0, may hold values from 1 to 128
Outputs:
- residual_vis: float32 [8, 256, 2, 128], P(('tile', 'beam'), ('bl', 'pol')), parts along dimension 0
- dirty_grid: float32 [8, 16384, 2, 128], P(('tile', 'beam'), ('bl', 'pol')), parts along dimension 0
The draws below stay inside these ranges and needn't reach their ends.
There are 2 independent parts, one for each index of `tile`. The reference program is written for one: setup_inputs(seed, part) draws one part's arguments, and reference() takes and returns one part's arrays. A program takes and returns all parts, laid end to end along the dimension named above; each array names one. Nothing has to cross between parts.
Inputs may be any that keep to these rules, and one draw needn't show every extreme that they name: `tile_owner`: among the 64 visibility tiles of one device, at most 32 name the same owner, and in some blocks one owner is named exactly 32 times.
All inputs are finite; a program needn't handle non-finite values.
Results may differ from the reference program's by a relative error of at most 0.0055.
Values may be sent and summed in bfloat16 or wider, within the bound.
A program may use at most 64 MiB of HBM per device.

```python
import math
import jax
import jax.numpy as jnp
import numpy as np
from jax import lax

GRID = 2048
TILE_VIS = 128
VIS_DEV = 64
BEAMS = 4
GROUP = 4
STRIDE = 1024
HALO = 512
SKY_COLS = 4096
TILES_DEV = 4096
TILES_ALL = 16384
VIS_ALL = 256
CAP = 32


def set_ends(values, own_key, smallest, top_value):
    extent = values.shape
    index_at = [jax.random.randint(jax.random.fold_in(own_key, axis), (), 0, extent[axis]) for axis in range(len(extent))]
    values = values.at[tuple(index_at)].set(smallest)
    longest = extent.index(max(extent))
    index_at[longest] = (index_at[longest] + 1) % extent[longest]
    return values.at[tuple(index_at)].set(top_value)


def steps_of(stream_key, extent, shards, smallest, high):
    factor_of = 1.0
    for position, parts in shards:
        heights = jax.random.uniform(jax.random.fold_in(jax.random.fold_in(stream_key, 6), position), (parts,), jnp.float32, smallest / len(shards), high / len(shards))
        factor_of = factor_of * jnp.repeat(jnp.exp(heights), extent[position] // parts).reshape((-1,) + (1,) * (len(extent) - 1 - position))
    return factor_of


def shared_out(stream_key, own, number, rows, number_of, top, limit, skew):
    sequence = jax.random.permutation(stream_key, number_of)
    heavy_load, ordinary = shares(number_of, rows * top, limit, skew, True), shares(number_of, rows * top, limit, skew, False)
    places = jnp.arange(number_of)

    def named(tallies, rotation):
        used = int((tallies > 0).sum())
        fixed = max(1, used // 4)
        passed = fixed + (places - fixed + rotation * (used - fixed)) % max(1, number_of - fixed)
        return jnp.zeros((number_of,), jnp.int32).at[sequence[jnp.where(places < fixed, places, passed)]].set(jnp.asarray(tallies, jnp.int32))

    tallies = jnp.where(number % 4 == 0, named(heavy_load, number // 4), named(ordinary, number - number // 4 - 1))
    mixed = jax.random.permutation(jax.random.fold_in(own, 3), number_of)
    donor, taker = mixed[0:number_of // 2 * 2:2], mixed[1:number_of // 2 * 2:2]
    room = jnp.minimum(tallies[donor] - 1, limit - tallies[taker]) // 2
    room = jnp.where((donor == sequence[0]) | (taker == sequence[0]) | (tallies[taker] == 0), 0, jnp.maximum(room, 0))
    passed = jax.random.randint(jax.random.fold_in(own, 4), (number_of // 2,), 0, 1 << 20) % (room + 1)
    tallies = tallies.at[donor].add(-passed).at[taker].add(passed)
    items = jnp.searchsorted(jnp.cumsum(tallies), jnp.arange(rows * top), side="right").astype(jnp.int32)
    listing = items.reshape(top, rows).T
    listing = listing[jax.random.permutation(jax.random.fold_in(own, 1), rows)]
    rotation = jax.random.randint(jax.random.fold_in(own, 2), (rows, 1), 0, top)
    return jnp.take_along_axis(listing, (jnp.arange(top)[None, :] + rotation) % top, axis=1)


def shares(count, total, limit, slope, full):
    weights = [(1 << 20) // math.isqrt(rank ** slope) + 1 for rank in range(1, count + 1)]
    largest = limit if full else min(limit, max(-(-total // count), total * weights[0] // sum(weights)))
    least = 1 if total - largest >= count - 1 else 0
    given, spare = [largest] + [least] * (count - 1), total - largest - least * (count - 1)
    while spare > 0:
        free = [i for i in range(1, count) if given[i] < largest] or [i for i in range(1, count) if given[i] < limit]
        pool, left = sum([weights[i] for i in free]), spare
        for i in free:
            extra = min(limit - given[i], max(1, left * weights[i] // pool), spare)
            given[i] = given[i] + extra
            spare = spare - extra
    return np.array(given)


def scatter_about(key, dims, spread, most, split=(), held_as=jnp.bfloat16):
    array = spread * jax.random.normal(key, dims, jnp.float32)
    if split:
        array = array * steps_of(key, dims, split, -0.22, 0.18)
    return jnp.clip(array, -most, most).astype(held_as)


def setup_inputs(seed: int = 0, part: int = 0) -> dict:
    arg_keys = jax.random.split(jax.random.key(seed), 8)
    part_keys = jax.random.split(jax.random.fold_in(arg_keys[7], part), 8)
    sky_model = scatter_about(part_keys[0], (GRID, SKY_COLS), 1.0, 6.0, ((0, 4), (1, 4)))
    beam_pattern = jnp.clip(0.099609375 + 0.9003906 * jax.random.uniform(part_keys[1], (BEAMS, GRID, GRID), jnp.float32) ** steps_of(part_keys[1], (BEAMS, GRID, GRID), ((0, 4), (1, 4)), -0.2, 0.2), 0.099609375, 1.0).astype(jnp.bfloat16)
    kernels = scatter_about(part_keys[2], (BEAMS, VIS_ALL, TILE_VIS, TILE_VIS), TILE_VIS ** -0.5, 0.5, ((0, 4), (1, 4)))
    observed = scatter_about(part_keys[3], (BEAMS, VIS_ALL, 2, TILE_VIS), 1.0, 6.0, ((0, 4), (1, 4)), jnp.float32)
    tile_owner_keys = jax.random.split(jax.random.fold_in(part_keys[4], 1), BEAMS * VIS_ALL // VIS_DEV)
    tile_owner_turns = jax.random.permutation(jax.random.fold_in(part_keys[4], 3), BEAMS * VIS_ALL // VIS_DEV)
    tile_owner = jax.vmap(lambda own, number: shared_out(jax.random.fold_in(part_keys[4], 2), own, number, VIS_DEV, GROUP, 1, CAP, 2))(tile_owner_keys, tile_owner_turns).reshape((BEAMS, VIS_ALL, 1))
    tile_local = set_ends(jax.random.randint(part_keys[5], (BEAMS, VIS_ALL), 0, TILES_DEV), jax.random.fold_in(part_keys[5], 1), 0, TILES_DEV - 1).astype(jnp.int32)
    vis_count = set_ends(jax.random.randint(part_keys[6], (BEAMS, VIS_ALL), 1, TILE_VIS + 1), jax.random.fold_in(part_keys[6], 1), 1, TILE_VIS).astype(jnp.int32)
    return {"sky_model": sky_model, "beam_pattern": beam_pattern, "kernels": kernels, "observed": observed, "tile_owner": tile_owner, "tile_local": tile_local, "vis_count": vis_count}


def tables(rows, cols):
    row_index = jnp.arange(rows, dtype=jnp.int32)[:, None]
    col_index = jnp.arange(cols, dtype=jnp.int32)[None, :]
    angles = (row_index * col_index % GRID).astype(jnp.float32) * jnp.float32(2.0 * math.pi / GRID)
    factor = jnp.float32(1.0 / math.sqrt(GRID))
    return ((jnp.cos(angles) * factor).astype(jnp.bfloat16), (jnp.sin(angles) * factor).astype(jnp.bfloat16))

def product(left, right):
    return jnp.dot(left.astype(jnp.float32), right.astype(jnp.float32), precision=lax.Precision.HIGHEST)

def reference(sky_model, beam_pattern, kernels, observed, tile_owner, tile_local, vis_count):
    cos_one, sin_one = tables(GRID // 2, GRID)
    cos_two, sin_two = tables(GRID, GRID)
    padded = jnp.pad(sky_model, ((0, 0), (HALO, HALO)))

    def one_beam(packed):
        beam_no, pattern, kernel_set, seen, owners, local_ids, counts = packed
        window = lax.dynamic_slice_in_dim(padded, (beam_no * STRIDE).astype(jnp.int32), GRID, 1)
        apparent = (pattern.astype(jnp.float32) * window.astype(jnp.float32)).astype(jnp.bfloat16)
        half_real = product(cos_one, apparent.T).astype(jnp.bfloat16)
        half_imag = (-product(sin_one, apparent.T)).astype(jnp.bfloat16)
        uv_real = product(half_real, cos_two) + product(half_imag, sin_two)
        uv_imag = product(half_imag, cos_two) - product(half_real, sin_two)
        uv_grid = jnp.stack([uv_real, uv_imag]).astype(jnp.bfloat16)
        uv_tiles = uv_grid.reshape(2, GRID // 16, 8, GRID // 16, 16).transpose(1, 3, 0, 2, 4).reshape(TILES_ALL, 2, TILE_VIS)
        tile_index = (owners * TILES_DEV + local_ids).astype(jnp.int32)
        fetched = uv_tiles[tile_index]
        kernel_wide = kernel_set.astype(jnp.float32)
        predicted = jnp.einsum('rjm,rcm->rcj', kernel_wide, fetched.astype(jnp.float32), precision=lax.Precision.HIGHEST)
        live_mask = jnp.arange(TILE_VIS, dtype=jnp.int32)[None, :] < counts[:, None]
        residual = jnp.where(live_mask[:, None, :], seen - predicted, jnp.zeros_like(predicted))
        residual_low = residual.astype(jnp.bfloat16)
        contribution = jnp.einsum('rjm,rcj->rcm', kernel_wide, residual_low.astype(jnp.float32), precision=lax.Precision.HIGHEST)
        dirty = jax.ops.segment_sum(contribution, tile_index, num_segments=TILES_ALL)
        return (residual, dirty)
    beam_numbers = jnp.arange(BEAMS, dtype=jnp.int32)
    residual_vis, dirty_grid = lax.map(one_beam, (beam_numbers, beam_pattern, kernels, observed, tile_owner[:, :, 0], tile_local, vis_count))
    return (residual_vis, dirty_grid)
```

```python
import functools
import math

import jax
import jax.numpy as jnp
import numpy as np
from jax import lax
from jax.experimental import pallas as pl
from jax.experimental.pallas import tpu as pltpu
from jax.sharding import PartitionSpec as P

MESH = pl.DeviceIdType.MESH
RADIX = 8
WIDE = 16
scope = jax.named_scope
VMEM = pl.BlockSpec(memory_space=pltpu.VMEM)
HBM = pl.BlockSpec(memory_space=pltpu.HBM)
NT = (((1,), (1,)), ((), ()))
NN = (((1,), (0,)), ((), ()))


def wave(rows, cols, period, factor):
    angle = (np.outer(rows, cols) % period) * (2.0 * math.pi / period)
    return np.cos(angle) * factor, np.sin(angle) * factor


def first_tables(grid):
    span = grid // RADIX
    blocks = grid // 2 // RADIX
    cols = np.arange(span)

    def of(i):
        return wave(RADIX * np.arange(blocks) + i, cols, grid, grid**-0.5)

    real = []
    for i in (0, RADIX // 2):
        cos, sin = of(i)
        real.append(np.concatenate([cos, -sin], 0))
    pairs = []
    for i in range(1, RADIX // 2):
        cos, sin = of(i)
        cos_m, sin_m = of(RADIX - i)
        pairs.append(
            np.concatenate(
                [
                    np.concatenate([cos, sin], 1),
                    np.concatenate([-sin, cos], 1),
                    np.concatenate([cos_m, -sin_m], 1),
                    np.concatenate([-sin_m, -cos_m], 1),
                ],
                0,
            )
        )
    return np.stack(real).astype(jnp.bfloat16), np.stack(pairs).astype(jnp.bfloat16)


def second_tables(grid):
    period = grid // WIDE
    phase = np.stack(wave(np.arange(period), np.arange(period), period, 1.0), 1)
    cos, sin = wave(np.arange(period), np.arange(WIDE), grid, grid**-0.5)
    fine = np.stack([np.tile(cos, (1, RADIX)), np.tile(sin, (1, RADIX))])
    cos, sin = wave(np.arange(WIDE), np.arange(WIDE), WIDE, 1.0)
    coarse = np.stack([np.tile(cos, (1, RADIX)), np.tile(sin, (1, RADIX))], 1)
    return phase.astype(np.float32), fine.astype(np.float32), coarse.astype(np.float32)


def group_index():
    return lax.axis_index("bl") * lax.axis_size("pol") + lax.axis_index("pol")


def chip_peer(turn, core):
    chips, cores = lax.axis_size("bl"), lax.axis_size("pol")
    chip = lax.rem(lax.axis_index("bl") + turn, chips)
    return chip, lax.rem(lax.axis_index("pol") + core, cores)


def transform_rows(at, pattern, strip, low, high, real_table, pair_table, g_real, g_pair, re, im):
    span = pattern.shape[1] // RADIX
    width = low.shape[1]
    inner = strip.shape[1]
    step = 32
    root = math.sqrt(0.5)

    def octant(a, src):
        first = a * span
        if first < width:
            return low[src, first : first + span]
        if first < width + inner:
            return strip[src, first - width : first - width + span]
        return high[src, first - width - inner : first - width - inner + span]

    def fold(index, carry):
        src = pl.ds(pl.multiple_of(at + index * step, step), step)
        dst = pl.ds(pl.multiple_of(index * step, step), step)
        parts = [
            (pattern[src, a * span : (a + 1) * span] * octant(a, src)).astype(jnp.float32) for a in range(RADIX)
        ]
        s = [parts[a] + parts[a + 4] for a in range(4)]
        d = [parts[a] - parts[a + 4] for a in range(4)]
        even, odd = s[0] + s[2], s[1] + s[3]
        near, far = root * (d[1] - d[3]), root * (d[1] + d[3])

        def put(ref, lead, off, value):
            ref[lead, dst, off : off + span] = value.astype(jnp.bfloat16)

        put(g_real, 0, 0, even + odd)
        put(g_real, 1, 0, even - odd)
        put(g_pair, 0, 0, d[0] + near)
        put(g_pair, 0, span, -(d[2] + far))
        put(g_pair, 1, 0, s[0] - s[2])
        put(g_pair, 1, span, s[3] - s[1])
        put(g_pair, 2, 0, d[0] - near)
        put(g_pair, 2, span, d[2] - far)
        return carry

    lax.fori_loop(0, g_real.shape[1] // step, fold, 0)
    blocks = re.shape[0]
    re = re.reshape(blocks * RADIX, re.shape[2])
    im = im.reshape(blocks * RADIX, im.shape[2])
    for k, i in enumerate((0, RADIX // 2)):
        out = lax.dot_general(real_table[k], g_real[k], NT, preferred_element_type=jnp.float32)
        re[pl.ds(i, blocks, stride=RADIX), :] = out[:blocks]
        im[pl.ds(i, blocks, stride=RADIX), :] = out[blocks:]
    for k in range(RADIX // 2 - 1):
        out = lax.dot_general(pair_table[k], g_pair[k], NT, preferred_element_type=jnp.float32)
        for n, (ref, i) in enumerate(((re, k + 1), (im, k + 1), (re, RADIX - 1 - k), (im, RADIX - 1 - k))):
            ref[pl.ds(i, blocks, stride=RADIX), :] = out[n * blocks : (n + 1) * blocks]


def turn_tiles(first, asker, codes, phase, re, im, turned_re, turned_im):
    period = phase.shape[2]
    sets = codes.shape[1]

    def turn_set(g, carry):
        base = pl.multiple_of((first * sets + g) * RADIX * RADIX, RADIX * RADIX)
        for n in range(RADIX):
            tile = codes[asker, g, n]
            turn = phase[jnp.bitwise_and(tile, period - 1)]
            cos, sin = turn[0:1], turn[1:2]
            up = lax.shift_right_logical(tile, period.bit_length() - 1)
            x, y = re[up], im[up]
            rows = pl.ds(base + n, RADIX, stride=RADIX)
            turned_re[rows, :] = x * cos + y * sin
            turned_im[rows, :] = y * cos - x * sin
        return carry

    lax.fori_loop(0, sets, turn_set, 0, unroll=True)


def pick_cells(weights, turned_re, turned_im):
    rows, cells = turned_re.shape
    turned = jnp.concatenate([turned_re[...], turned_im[...]], axis=1).astype(jnp.bfloat16)
    cells_of = lax.dot_general(turned, weights, NN, preferred_element_type=jnp.float32)
    wide = cells_of.shape[1]
    cells_of = cells_of.reshape(rows // (RADIX * RADIX), RADIX, RADIX, wide)
    column = lax.broadcasted_iota(jnp.int32, (RADIX, wide), 1)
    row_of = (column % (wide // 2)) // WIDE
    picked = cells_of[:, 0]
    for i in range(1, RADIX):
        picked = jnp.where((row_of == i)[None], cells_of[:, i], picked)
    return picked.reshape(rows // RADIX, wide)


def predict_kernel(
    group, beams, tiles_dev,
    sky, pattern_in, kernels_in, observed_in, owner_in, place_in, counts_in, real_in, pair_in, phase_in, fine_in,
    coarse_in,
    residual, shared, hot,
    strip, low, high, pattern, kernels, observed, owner, place, counts, real_table, pair_table, phase, fine, coarse,
    table, code, codes, codes_s,
    g_real, g_pair, re, im, turned_re, turned_im, total, part, came, given, wide, narrow,
    local, halo_send, halo_recv, code_send, code_recv, part_send, part_recv, share_send, share_recv,
):
    beam = lax.axis_index("beam")
    me = group_index()
    vis, cells = kernels.shape[0], kernels.shape[1]
    width = low.shape[1]
    period = phase.shape[2]
    chunks = pattern.shape[0] // period
    chips, cores = lax.axis_size("bl"), lax.axis_size("pol")
    has_next, has_last = beam < beams - 1, beam > 0

    names = ("strip", "owner", "place", "phase", "fine", "coarse", "pattern", "real", "pair", "kernels", "observed", "counts")
    loads = {}
    for n, (name, src, dst) in enumerate(zip(names, (
        sky, owner_in, place_in, phase_in, fine_in, coarse_in.at[pl.ds(me * chunks, chunks)], pattern_in, real_in,
        pair_in, kernels_in, observed_in, counts_in,
    ), (
        strip, owner, place, phase, fine, coarse, pattern, real_table, pair_table, kernels, observed, counts,
    ))):
        loads[name] = pltpu.make_async_copy(src, dst, local.at[n])
        loads[name].start()

    orders = [(turn, core) for turn in range(1, chips + 1) for core in range(cores) if turn < chips or core > 0]
    barrier = pltpu.get_barrier_semaphore()

    def greet(device):
        pl.semaphore_signal(barrier, inc=1, device_id=device, device_id_type=MESH)

    for turn, core in orders:
        chip, side = chip_peer(turn, core)
        greet({"bl": chip, "pol": side})

    @pl.when(has_next)
    def _():
        greet({"beam": beam + 1})

    @pl.when(has_last)
    def _():
        greet({"beam": beam - 1})

    @pl.when(beam == 0)
    def _():
        low[...] = jnp.zeros_like(low)

    @pl.when(beam == beams - 1)
    def _():
        high[...] = jnp.zeros_like(high)

    total[...] = jnp.zeros_like(total)
    wide[...] = jnp.zeros_like(wide)
    loads["owner"].wait()
    loads["place"].wait()
    named = owner[...] * tiles_dev + place[...]
    named = jnp.concatenate([named] * (code.shape[1] // vis), axis=1)
    for g in range(vis // RADIX):
        code[g : g + 1, :] = named if g == 0 else pltpu.roll(named, code.shape[1] - g * RADIX, 1)
    loads["fine"].wait()
    loads["coarse"].wait()
    for k in range(chunks):
        cos_c, sin_c = coarse[k, 0:1], coarse[k, 1:2]
        cos = (fine[0] * cos_c - fine[1] * sin_c).astype(jnp.bfloat16)
        sin = (fine[1] * cos_c + fine[0] * sin_c).astype(jnp.bfloat16)
        table[k, :period, :cells] = cos
        table[k, :period, cells:] = -sin
        table[k, period:, :cells] = sin
        table[k, period:, cells:] = cos
    loads["strip"].wait()

    edges = jnp.where(beam < beams - 1, 1, 0) + jnp.where(beam > 0, 1, 0)
    with scope("barrier"):
        pl.semaphore_wait(barrier, group - 1 + edges)

    def halo(side, k):
        rows = pl.ds(pl.multiple_of(k * period, period), period)
        first = 0 if side else strip.shape[1] - width
        return pltpu.make_async_remote_copy(
            src_ref=strip.at[rows, pl.ds(first, width)], dst_ref=(high if side else low).at[rows, :],
            send_sem=halo_send.at[side, k], recv_sem=halo_recv.at[side, k],
            device_id={"beam": beam - 1 if side else beam + 1}, device_id_type=MESH,
        )

    def to_peer(turn, core, source, target, send, recv):
        chip, side = chip_peer(turn, core)
        slot = (turn - 1) * cores + core
        return pltpu.make_async_remote_copy(
            src_ref=source, dst_ref=target,
            send_sem=send.at[slot], recv_sem=recv.at[slot],
            device_id={"bl": chip, "pol": side}, device_id_type=MESH,
        )

    def index_of(turn, core):
        chip, side = chip_peer(turn, core)
        return chip * cores + side

    named_copies = [to_peer(turn, core, code, codes.at[me], code_send, code_recv) for turn, core in orders]
    for copy in named_copies:
        copy.start()

    @pl.when(has_next)
    def _():
        for k in range(chunks):
            halo(0, k).start()

    @pl.when(has_last)
    def _():
        for k in range(chunks):
            halo(1, k).start()

    codes[me] = code[...]
    with scope("codes"):
        for copy in named_copies:
            copy.wait()
    to_scalar = pltpu.make_async_copy(codes, codes_s, local.at[len(loads)])
    to_scalar.start()

    lanes = code.shape[1]
    each = lanes // vis
    lane = lax.broadcasted_iota(jnp.int32, (1, lanes), 1)
    keys = []
    for first in range(0, group, each):
        key = codes[first, 0:1, :]
        for n in range(1, each):
            key = jnp.where(lane < n * vis, key, codes[first + n, 0:1, :])
        keys.append(key)
    key = jnp.concatenate(keys, axis=1) - me * tiles_dev
    step = 256

    def heat(block, carry):
        at = pl.multiple_of(block * step, step)
        tile = lax.broadcasted_iota(jnp.int32, (step, key.shape[1]), 0)
        hot[pl.ds(at, step), :] = jnp.where(tile == key - at, 1.0, 0.0).astype(jnp.bfloat16)
        return carry

    with scope("heat"):
        lax.fori_loop(0, tiles_dev // step, heat, 0)
    to_scalar.wait()
    for name in ("phase", "pattern", "real", "pair"):
        loads[name].wait()

    def of_chunk(k, carry):
        with scope("halo"):

            @pl.when(has_last)
            def _():
                halo(0, k).wait_recv()

            @pl.when(has_next)
            def _():
                halo(1, k).wait_recv()

        with scope("rows"):
            transform_rows(k * period, pattern, strip, low, high, real_table, pair_table, g_real, g_pair, re, im)

        def of_chip(turn, inner):
            with scope("turn"):
                for core in range(cores):
                    turn_tiles(core, index_of(turn, core), codes_s, phase, re, im, turned_re, turned_im)
            picked = pick_cells(table[k], turned_re, turned_im)
            for core in range(cores):
                rows = pl.ds(pl.multiple_of(index_of(turn, core) * vis, vis), vis)
                total[rows, :] += picked[core * vis : (core + 1) * vis]

                @pl.when((k == chunks - 1) & ((turn < chips) | (core > 0)))
                def _():
                    part[rows, :] = total[rows, :].astype(part.dtype)
                    to_peer(turn, core, part.at[rows, :], came.at[me], part_send, part_recv).start()

            return inner

        lax.fori_loop(1, chips + 1, of_chip, 0)
        return carry

    lax.fori_loop(0, chunks, of_chunk, 0)

    loads["counts"].wait()
    loads["observed"].wait()
    own = lax.broadcasted_iota(jnp.int32, (vis, vis), 0) == lax.broadcasted_iota(jnp.int32, (vis, vis), 1)
    count = jnp.sum(jnp.where(own, counts[...].astype(jnp.float32), 0.0), axis=1, keepdims=True)
    mask = lax.broadcasted_iota(jnp.int32, (vis, cells), 1).astype(jnp.float32) < count
    mine = total[pl.ds(pl.multiple_of(me * vis, vis), vis), :]
    loads["kernels"].wait()
    with scope("parts"):
        for turn, core in orders:
            rows = pl.ds(pl.multiple_of(index_of(turn, core) * vis, vis), vis)
            to_peer(turn, core, part.at[rows, :], came.at[me], part_send, part_recv).wait()
    for turn, core in orders:
        mine = mine + came[index_of(turn, core)].astype(jnp.float32)
    for c in range(2):
        wide[pl.ds(c, vis, stride=RADIX), :] = mine[:, c * cells : (c + 1) * cells]

    def apply(dims):
        def of_tile(r, carry):
            at = pl.ds(pl.multiple_of(r * RADIX, RADIX), RADIX)
            narrow[at, :] = lax.dot_general(
                wide[at, :].astype(jnp.bfloat16), kernels[r], dims, preferred_element_type=jnp.float32
            )
            return carry

        lax.fori_loop(0, vis, of_tile, 0, unroll=True)

    with scope("nt"):
        apply(NT)
    for c in range(2):
        seen = observed[pl.ds(c, vis, stride=2), :]
        left = jnp.where(mask, seen - narrow[pl.ds(c, vis, stride=RADIX), :], 0.0)
        residual[pl.ds(c, vis, stride=2), :] = left
        wide[pl.ds(c, vis, stride=RADIX), :] = left
    with scope("nn"):
        apply(NN)
    for c in range(2):
        given[:, c * cells : (c + 1) * cells] = narrow[pl.ds(c, vis, stride=RADIX), :].astype(given.dtype)
    given_copies = [to_peer(turn, core, given, shared.at[me], share_send, share_recv) for turn, core in orders]
    for copy in given_copies:
        copy.start()
    shared[me] = given[...]
    with scope("given"):
        for copy in given_copies:
            copy.wait()

    @pl.when(has_next)
    def _():
        for k in range(chunks):
            halo(0, k).wait_send()

    @pl.when(has_last)
    def _():
        for k in range(chunks):
            halo(1, k).wait_send()


def dirty_kernel(hot, terms, left, dirty, residual, held, sems):
    blocks, rows, cells = held.shape
    rows = rows // 2
    kept = pltpu.make_async_copy(left, residual, sems.at[blocks])
    kept.start()
    copies = [kept]
    for block in range(blocks):
        out = lax.dot_general(
            hot[block * rows : (block + 1) * rows, :], terms[...], NN, preferred_element_type=jnp.float32
        )
        for c in range(2):
            held[block, pl.ds(c, rows, stride=2), :] = out[:, c * cells : (c + 1) * cells]
        copy = pltpu.make_async_copy(
            held.at[block], dirty.at[pl.ds(block * rows * 2, rows * 2), :], sems.at[block]
        )
        copy.start()
        copies.append(copy)
    for copy in copies:
        copy.wait()


def on_device(sky_model, beam_pattern, kernels, observed, tile_owner, tile_local, vis_count):
    group = lax.axis_size(("bl", "pol"))
    cores = lax.axis_size("pol")
    beams = lax.axis_size("beam")
    rows, grid = beam_pattern.shape[1:]
    strip = sky_model.shape[1]
    halo = (grid - strip) // 2
    vis, cells = kernels.shape[1], kernels.shape[3]
    tiles_dev = (grid // 2 // RADIX) * (grid // WIDE) // group
    lanes = 128
    f32, bf16, i32 = jnp.float32, jnp.bfloat16, jnp.int32
    real_table, pair_table = first_tables(grid)
    phase, fine, coarse = second_tables(grid)
    span, period = grid // RADIX, grid // WIDE
    chunks = rows // period
    dma = pltpu.SemaphoreType.DMA
    arrays = (
        sky_model, beam_pattern[0], kernels[0], observed.reshape(vis * 2, cells),
        tile_owner.reshape(1, vis), tile_local, vis_count,
        jnp.asarray(real_table), jnp.asarray(pair_table), jnp.asarray(phase), jnp.asarray(fine), jnp.asarray(coarse),
    )

    residual, shared, hot = pl.pallas_call(
        functools.partial(predict_kernel, group, beams, tiles_dev),
        out_shape=(
            pltpu.VMEM((vis * 2, cells), f32),
            pltpu.VMEM((group, vis, 2 * cells), bf16),
            pltpu.VMEM((tiles_dev, group * vis), bf16),
        ),
        in_specs=[HBM] * len(arrays),
        out_specs=(VMEM, VMEM, VMEM),
        scratch_shapes=[
            pltpu.VMEM((rows, strip), bf16),
            pltpu.VMEM((rows, halo), bf16),
            pltpu.VMEM((rows, halo), bf16),
            pltpu.VMEM((rows, grid), bf16),
            pltpu.VMEM((vis, cells, cells), bf16),
            pltpu.VMEM((vis * 2, cells), f32),
            pltpu.VMEM((1, vis), i32),
            pltpu.VMEM((1, vis), i32),
            pltpu.VMEM((1, vis), i32),
            pltpu.VMEM(real_table.shape, bf16),
            pltpu.VMEM(pair_table.shape, bf16),
            pltpu.VMEM(phase.shape, f32),
            pltpu.VMEM(fine.shape, f32),
            pltpu.VMEM((chunks, *coarse.shape[1:]), f32),
            pltpu.VMEM((chunks, 2 * period, 2 * cells), bf16),
            pltpu.VMEM((vis // RADIX, lanes), i32),
            pltpu.VMEM((group, vis // RADIX, lanes), i32),
            pltpu.SMEM((group, vis // RADIX, lanes), i32),
            pltpu.VMEM((2, period, span), bf16),
            pltpu.VMEM((RADIX // 2 - 1, period, 2 * span), bf16),
            pltpu.VMEM((grid // 2 // RADIX, RADIX, period), f32),
            pltpu.VMEM((grid // 2 // RADIX, RADIX, period), f32),
            pltpu.VMEM((cores * vis * RADIX, period), f32),
            pltpu.VMEM((cores * vis * RADIX, period), f32),
            pltpu.VMEM((group * vis, 2 * cells), f32),
            pltpu.VMEM((group * vis, 2 * cells), bf16),
            pltpu.VMEM((group, vis, 2 * cells), bf16),
            pltpu.VMEM((vis, 2 * cells), bf16),
            pltpu.VMEM((vis * RADIX, cells), f32),
            pltpu.VMEM((vis * RADIX, cells), f32),
            dma((len(arrays) + 1,)),
            dma((2, chunks)), dma((2, chunks)),
            dma((group,)), dma((group,)),
            dma((group,)), dma((group,)),
            dma((group,)), dma((group,)),
        ],
        compiler_params=pltpu.CompilerParams(
            collective_id=0, has_side_effects=True, vmem_limit_bytes=40 * 1024 * 1024
        ),
        name="predict",
    )(*[pltpu.with_memory_space_constraint(x, pltpu.HBM) for x in arrays])

    blocks = 8
    dirty, residual = pl.pallas_call(
        dirty_kernel,
        out_shape=(
            jax.ShapeDtypeStruct((tiles_dev * 2, cells), f32),
            jax.ShapeDtypeStruct((vis * 2, cells), f32),
        ),
        in_specs=[VMEM, VMEM, VMEM],
        out_specs=(HBM, HBM),
        scratch_shapes=[pltpu.VMEM((blocks, tiles_dev * 2 // blocks, cells), f32), dma((blocks + 1,))],
        compiler_params=pltpu.CompilerParams(vmem_limit_bytes=12 * 1024 * 1024),
        name="dirty",
    )(hot, shared.reshape(group * vis, 2 * cells), residual)
    return (
        residual.reshape(1, vis, 2, cells),
        dirty.reshape(1, tiles_dev, 2, cells),
    )


def solution(mesh):
    placed = (
        P(("tile", "bl", "pol"), "beam"),
        P(("tile", "beam"), ("bl", "pol"), None),
        P(("tile", "beam"), ("bl", "pol"), None, None),
        P(("tile", "beam"), ("bl", "pol"), None, None),
        P(("tile", "beam"), ("bl", "pol"), None),
        P(("tile", "beam"), ("bl", "pol")),
        P(("tile", "beam"), ("bl", "pol")),
    )
    return jax.shard_map(
        on_device,
        mesh=mesh,
        in_specs=placed,
        out_specs=(
            P(("tile", "beam"), ("bl", "pol"), None, None),
            P(("tile", "beam"), ("bl", "pol"), None, None),
        ),
        check_vma=False,
    )
```

```python
import functools
import math

import jax
import jax.numpy as jnp
import numpy as np
from jax import lax
from jax.experimental import pallas as pl
from jax.experimental.pallas import tpu as pltpu
from jax.sharding import PartitionSpec as P

MESH = pl.DeviceIdType.MESH
RADIX = 8
WIDE = 16
PITCH = RADIX + 1
PIECES = 2
scope = jax.named_scope
VMEM = pl.BlockSpec(memory_space=pltpu.VMEM)
HBM = pl.BlockSpec(memory_space=pltpu.HBM)
NT = (((1,), (1,)), ((), ()))
NN = (((1,), (0,)), ((), ()))
TN = (((0,), (0,)), ((), ()))


def wave(rows, cols, period, factor):
    angle = (np.outer(rows, cols) % period) * (2.0 * math.pi / period)
    return np.cos(angle) * factor, np.sin(angle) * factor


def first_tables(grid):
    span = grid // RADIX
    blocks = grid // 2 // RADIX
    cols = np.arange(span)

    def of(i):
        return wave(RADIX * np.arange(blocks) + i, cols, grid, grid**-0.5)

    real = []
    for i in (0, RADIX // 2):
        cos, sin = of(i)
        real.append(np.concatenate([cos, -sin], 0))
    tables = [np.concatenate(real, 1)]
    for i in range(1, RADIX // 2):
        cos, sin = of(i)
        cos_m, sin_m = of(RADIX - i)
        tables.append(
            np.concatenate(
                [
                    np.concatenate([cos, sin], 1),
                    np.concatenate([-sin, cos], 1),
                    np.concatenate([cos_m, -sin_m], 1),
                    np.concatenate([-sin_m, -cos_m], 1),
                ],
                0,
            )
        )
    return np.concatenate(tables, 0).astype(jnp.bfloat16)


def second_tables(grid):
    period = grid // WIDE
    phase = np.stack(wave(np.arange(period), np.arange(period), period, 1.0), 1)
    cos, sin = wave(np.arange(period), np.arange(WIDE), grid, grid**-0.5)
    fine = [np.tile(cos, (1, RADIX)), np.tile(sin, (1, RADIX))]
    cos, sin = wave(np.arange(WIDE), np.arange(WIDE), WIDE, 1.0)
    coarse = np.stack([np.tile(cos, (1, RADIX)), np.tile(sin, (1, RADIX))], 1)
    waves = [phase.reshape(2 * period, -1), *fine, coarse.reshape(2 * WIDE, -1)]
    return np.concatenate(waves, 0).astype(np.float32)


def group_index():
    return lax.axis_index("bl") * lax.axis_size("pol") + lax.axis_index("pol")


class Slots:
    def __init__(self):
        self.chips, self.cores = lax.axis_size("bl"), lax.axis_size("pol")
        self.all = [(turn, core) for turn in range(1, self.chips + 1) for core in range(self.cores)]
        self.own = (self.chips, 0)
        self.peers = [pair for pair in self.all if pair != self.own]

    def number(self, pair):
        return (pair[0] - 1) * self.cores + pair[1]

    def device(self, pair):
        chip = lax.rem(lax.axis_index("bl") + pair[0], self.chips)
        return {"bl": chip, "pol": lax.rem(lax.axis_index("pol") + pair[1], self.cores)}

    def back(self, pair):
        turn = self.chips - pair[0] if pair[0] < self.chips else self.chips
        return turn, (self.cores - pair[1]) % self.cores


def transform_rows(at, pattern, strip, low, high, tables, g_real, g_pair, half):
    span = pattern.shape[1] // RADIX
    width = low.shape[1]
    inner = strip.shape[1]
    step = 32
    root = math.sqrt(0.5)

    def octant(a, src):
        first = a * span
        if first < width:
            return low[src, first : first + span]
        if first < width + inner:
            return strip[src, first - width : first - width + span]
        return high[src, first - width - inner : first - width - inner + span]

    def fold(index, carry):
        src = pl.ds(pl.multiple_of(at + index * step, step), step)
        dst = pl.ds(pl.multiple_of(index * step, step), step)
        parts = [
            (pattern[src, a * span : (a + 1) * span] * octant(a, src)).astype(jnp.float32) for a in range(RADIX)
        ]
        s = [parts[a] + parts[a + 4] for a in range(4)]
        d = [parts[a] - parts[a + 4] for a in range(4)]
        even, odd = s[0] + s[2], s[1] + s[3]
        near, far = root * (d[1] - d[3]), root * (d[1] + d[3])

        def put(ref, lead, off, value):
            ref[lead, dst, off : off + span] = value.astype(jnp.bfloat16)

        put(g_real, 0, 0, even + odd)
        put(g_real, 1, 0, even - odd)
        put(g_pair, 0, 0, d[0] + near)
        put(g_pair, 0, span, -(d[2] + far))
        put(g_pair, 1, 0, s[0] - s[2])
        put(g_pair, 1, span, s[3] - s[1])
        put(g_pair, 2, 0, d[0] - near)
        put(g_pair, 2, span, d[2] - far)
        return carry

    lax.fori_loop(0, g_real.shape[1] // step, fold, 0)
    blocks = half.shape[1] // PITCH
    re, im = half.at[0], half.at[1]
    for k, i in enumerate((0, RADIX // 2)):
        weights = tables[: 2 * blocks, k * span : (k + 1) * span]
        out = lax.dot_general(weights, g_real[k], NT, preferred_element_type=jnp.float32)
        re[pl.ds(i, blocks, stride=PITCH), :] = out[:blocks]
        im[pl.ds(i, blocks, stride=PITCH), :] = out[blocks:]
    for k in range(RADIX // 2 - 1):
        weights = tables[(2 + 4 * k) * blocks : (6 + 4 * k) * blocks]
        out = lax.dot_general(weights, g_pair[k], NT, preferred_element_type=jnp.float32)
        for n, (ref, i) in enumerate(((re, k + 1), (im, k + 1), (re, RADIX - 1 - k), (im, RADIX - 1 - k))):
            ref[pl.ds(i, blocks, stride=PITCH), :] = out[n * blocks : (n + 1) * blocks]


def turn_tiles(source, sets, codes, waves, half, turned_re, turned_im):
    lanes = codes.shape[2]

    def turn_set(g, carry):
        base = g * RADIX * PITCH
        for n in range(RADIX):
            at = codes[source, sets[0] + g, lanes // 2 + n]
            up = codes[source, sets[0] + g, n]
            cos, sin = waves[pl.ds(at, 1), :], waves[pl.ds(at + 1, 1), :]
            x, y = half[0, pl.ds(up, RADIX), :], half[1, pl.ds(up, RADIX), :]
            rows = pl.ds(base + n, RADIX, stride=PITCH)
            turned_re[rows, :] = x * cos + y * sin
            turned_im[rows, :] = y * cos - x * sin
        return carry

    lax.fori_loop(0, sets[1] - sets[0], turn_set, 0, unroll=True)


def pick_cells(count, weights, turned_re, turned_im):
    def rows_of(ref):
        return jnp.concatenate([ref[n * PITCH : n * PITCH + RADIX, :] for n in range(count * RADIX)], axis=0)

    turned = jnp.concatenate([rows_of(turned_re), rows_of(turned_im)], axis=1).astype(jnp.bfloat16)
    cells_of = lax.dot_general(turned, weights, NN, preferred_element_type=jnp.float32)
    wide = cells_of.shape[1]
    cells_of = cells_of.reshape(count, RADIX, RADIX, wide)
    column = lax.broadcasted_iota(jnp.int32, (RADIX, wide), 1)
    row_of = (column % (wide // 2)) // WIDE
    picked = cells_of[:, 0]
    for i in range(1, RADIX):
        picked = jnp.where((row_of == i)[None], cells_of[:, i], picked)
    return picked.reshape(count * RADIX, wide)


def predict_kernel(
    group, beams, tiles_dev,
    sky, pattern_in, kernels_in, observed_in, owner_in, place_in, counts_in, tables_in, waves_in,
    residual, shared, hot,
    strip, low, high, pattern, kernels, observed, owner, place, counts, counts_s, tables, waves,
    table, code, codes, split, codes_s,
    g_real, g_pair, half, turned_re, turned_im, total, part, came, given, wide, narrow, seen_wide, seen_rows, gram,
    local, halo_send, halo_recv, peer_send, code_recv, part_recv, share_recv,
):
    beam = lax.axis_index("beam")
    me = group_index()
    slots = Slots()
    vis, cells = kernels.shape[0], kernels.shape[1]
    width = low.shape[1]
    period = table.shape[1] // 2
    chunks = pattern.shape[0] // period
    has_next, has_last = beam < beams - 1, beam > 0

    strips = []
    for k in range(chunks):
        rows = pl.ds(k * period, period)
        strips.append(pltpu.make_async_copy(sky.at[rows], strip.at[rows], local.at[k]))
        strips[k].start()

    barrier = pltpu.get_barrier_semaphore()

    def greet(device):
        pl.semaphore_signal(barrier, inc=1, device_id=device, device_id_type=MESH)

    @pl.when(has_next)
    def _():
        greet({"beam": beam + 1})

    @pl.when(has_last)
    def _():
        greet({"beam": beam - 1})

    for pair in slots.peers:
        greet(slots.device(pair))

    loads = {}
    for n, (name, src, dst) in enumerate((
        ("owner", owner_in, owner), ("place", place_in, place), ("kernels", kernels_in, kernels),
        ("observed", observed_in, observed), ("counts", counts_in, counts), ("counts_s", counts_in, counts_s),
        ("waves", waves_in, waves), ("pattern", pattern_in, pattern), ("tables", tables_in, tables),
    )):
        loads[name] = pltpu.make_async_copy(src, dst, local.at[chunks + n])
        loads[name].start()

    strips[0].wait()
    edges = jnp.where(beam < beams - 1, 1, 0) + jnp.where(beam > 0, 1, 0)
    with scope("barrier"):
        pl.semaphore_wait(barrier, group - 1 + edges)

    def halo(side, k, count=1):
        rows = pl.ds(pl.multiple_of(k * period, period), count * period)
        first = 0 if side else strip.shape[1] - width
        return pltpu.make_async_remote_copy(
            src_ref=strip.at[rows, pl.ds(first, width)], dst_ref=(high if side else low).at[rows, :],
            send_sem=halo_send.at[side], recv_sem=halo_recv.at[side, k],
            device_id={"beam": beam - 1 if side else beam + 1}, device_id_type=MESH,
        )

    def to_peer(pair, piece, source, target, recv):
        n = slots.peers.index(pair)
        return pltpu.make_async_remote_copy(
            src_ref=source, dst_ref=target, send_sem=peer_send.at[piece, n], recv_sem=recv.at[piece, n],
            device_id=slots.device(pair), device_id_type=MESH,
        )

    early = lax.axis_index("pol") == 0
    for k in range(chunks):
        if k > 0:
            strips[k].wait()

        @pl.when(has_next & early)
        def _():
            halo(0, k).start()

        @pl.when(has_last & early)
        def _():
            halo(1, k).start()

    loads["owner"].wait()
    loads["place"].wait()
    named = owner[...] * tiles_dev + place[...]
    named = jnp.concatenate([named] * (code.shape[1] // vis), axis=1)
    for g in range(vis // RADIX):
        code[g : g + 1, :] = named if g == 0 else pltpu.roll(named, code.shape[1] - g * RADIX, 1)
    code_copies = [to_peer(pair, 0, code, codes.at[slots.number(pair)], code_recv) for pair in slots.peers]
    for copy in code_copies:
        copy.start()
    for k in range(chunks):

        @pl.when(has_next & jnp.logical_not(early))
        def _():
            halo(0, k).start()

        @pl.when(has_last & jnp.logical_not(early))
        def _():
            halo(1, k).start()

    codes[slots.number(slots.own)] = code[...]

    @pl.when(beam == 0)
    def _():
        low[...] = jnp.zeros_like(low)

    @pl.when(beam == beams - 1)
    def _():
        high[...] = jnp.zeros_like(high)

    total[...] = jnp.zeros_like(total)
    wide[...] = jnp.zeros_like(wide)
    seen_wide[...] = jnp.zeros_like(seen_wide)
    for name in ("waves", "kernels", "observed", "counts", "counts_s"):
        loads[name].wait()
    def spread(ref, first, count, c, value):
        rough = value.astype(jnp.bfloat16).astype(jnp.float32)
        ref[pl.ds(first * RADIX + c, count, stride=RADIX), :] = rough
        ref[pl.ds(first * RADIX + 2 + c, count, stride=RADIX), :] = value - rough

    def gathered(ref, first, count, c):
        rows = [ref[pl.ds(first * RADIX + c + d, count, stride=RADIX), :] for d in (0, 2)]
        return rows[0] + rows[1]

    def apply(matrices, dims, first, count):
        def of_tile(r, carry):
            at = pl.ds(pl.multiple_of(r * RADIX, RADIX), RADIX)
            narrow[at, :] = lax.dot_general(
                wide[at, :].astype(jnp.bfloat16), matrices[r], dims, preferred_element_type=jnp.float32
            )
            return carry

        lax.fori_loop(first, first + count, of_tile, 0, unroll=True)

    for k in range(chunks):
        row = 4 * period + 2 * (me * chunks + k)
        cos_c, sin_c = waves[pl.ds(row, 1), :], waves[pl.ds(row + 1, 1), :]
        cos_f, sin_f = waves[2 * period : 3 * period, :], waves[3 * period : 4 * period, :]
        cos = (cos_f * cos_c - sin_f * sin_c).astype(jnp.bfloat16)
        sin = (sin_f * cos_c + cos_f * sin_c).astype(jnp.bfloat16)
        table[k, :period, :cells] = cos
        table[k, :period, cells:] = -sin
        table[k, period:, :cells] = sin
        table[k, period:, cells:] = cos

    for c in range(2):
        spread(seen_wide, 0, vis, c, observed[pl.ds(c, vis, stride=2), :])
    row = lax.broadcasted_iota(jnp.int32, (cells, cells), 0)

    def gram_of(r, carry):
        at = pl.ds(pl.multiple_of(r * RADIX, RADIX), RADIX)
        kernel = kernels[r]
        live = jnp.where(row < counts_s[0, r], kernel.astype(jnp.float32), 0.0).astype(jnp.bfloat16)
        gram[r] = lax.dot_general(kernel, live, TN, preferred_element_type=jnp.float32).astype(jnp.bfloat16)
        seen_rows[at, :] = lax.dot_general(
            seen_wide[at, :].astype(jnp.bfloat16), live, NN, preferred_element_type=jnp.float32
        )
        return carry

    with scope("gram"):
        lax.fori_loop(0, vis, gram_of, 0, unroll=4)
    with scope("codes"):
        for copy in code_copies:
            copy.wait()
    lanes = code.shape[1]
    lane = lax.broadcasted_iota(jnp.int32, codes.shape, 2)
    up = lax.shift_right_logical(codes[...], period.bit_length() - 1)
    split[...] = jnp.where(lane < lanes // 2, up * PITCH, (codes[...] & (period - 1)) * 2)
    to_scalar = pltpu.make_async_copy(split, codes_s, local.at[0])
    to_scalar.start()

    fit = lanes // vis
    lane = lax.broadcasted_iota(jnp.int32, (1, lanes), 1)
    keys = []
    for first in range(0, group, fit):
        key = codes[first, 0:1, :]
        for n in range(1, fit):
            key = jnp.where(lane < n * vis, key, codes[first + n, 0:1, :])
        keys.append(key)
    key = jnp.concatenate(keys, axis=1) - me * tiles_dev
    step = 256

    def heat(block, carry):
        at = pl.multiple_of(block * step, step)
        tile = lax.broadcasted_iota(jnp.int32, (step, key.shape[1]), 0)
        hot[pl.ds(at, step), :] = jnp.where(tile == key - at, 1.0, 0.0).astype(jnp.bfloat16)
        return carry

    with scope("heat"):
        lax.fori_loop(0, tiles_dev // step, heat, 0)
    to_scalar.wait()
    for name in ("pattern", "tables"):
        loads[name].wait()

    each = vis // PIECES

    def span_of(pair, piece):
        first = slots.number(pair) * vis + piece * each
        return slice(first, first + each)

    def part_copy(pair, piece):
        target = came.at[slots.number(pair), pl.ds(piece * each, each)]
        return to_peer(pair, piece, part.at[span_of(pair, piece)], target, part_recv)

    def of_chunk(k, last):
        with scope("halo"):

            @pl.when(has_last)
            def _():
                halo(0, k).wait_recv()

            @pl.when(has_next)
            def _():
                halo(1, k).wait_recv()

        with scope("rows"):
            transform_rows(k * period, pattern, strip, low, high, tables, g_real, g_pair, half)
        far = [pair for pair in slots.all if pair[0] < slots.chips]
        near = [pair for pair in slots.all if pair[0] == slots.chips]
        for piece, pair in [(p, q) for some in (far, near) for p in range(PIECES) for q in some]:
            rows = span_of(pair, piece)
            at = slice(rows.start * PITCH, rows.stop * PITCH)
            re, im = turned_re.at[at], turned_im.at[at]
            sets = (piece * each // RADIX, (piece + 1) * each // RADIX)
            turn_tiles(slots.number(slots.back(pair)), sets, codes_s, waves, half, re, im)
            sums = total[rows, :] + pick_cells(each // RADIX, table[k], re, im)
            if last and pair != slots.own:
                part[rows, :] = sums.astype(part.dtype)
                part_copy(pair, piece).start()
            else:
                total[rows, :] = sums

    def chunk_loop(k, carry):
        of_chunk(k, False)
        return carry

    lax.fori_loop(0, chunks - 1, chunk_loop, 0)
    of_chunk(chunks - 1, True)

    given_copies = []
    for piece in range(PIECES):
        first = piece * each
        mine = total[span_of(slots.own, piece), :]
        with scope("parts"):
            for pair in slots.peers:
                part_copy(pair, piece).wait()
        for pair in slots.peers:
            mine = mine + came[slots.number(pair), first : first + each].astype(jnp.float32)
        for c in range(2):
            spread(wide, first, each, c, mine[:, c * cells : (c + 1) * cells])
        with scope("nn"):
            apply(gram, NN, first, each)
        for c in range(2):
            change = gathered(seen_rows, first, each, c) - gathered(narrow, first, each, c)
            given[first : first + each, c * cells : (c + 1) * cells] = change.astype(given.dtype)
        for pair in slots.peers:
            rows = pl.ds(first, each)
            copy = to_peer(pair, piece, given.at[rows], shared.at[slots.number(pair), rows], share_recv)
            copy.start()
            given_copies.append(copy)
        shared[slots.number(slots.own), first : first + each] = given[first : first + each]

    with scope("nt"):
        apply(kernels, NT, 0, vis)
    eye = lax.broadcasted_iota(jnp.int32, (vis, vis), 0) == lax.broadcasted_iota(jnp.int32, (vis, vis), 1)
    count = jnp.sum(jnp.where(eye, counts[...].astype(jnp.float32), 0.0), axis=1, keepdims=True)
    mask = lax.broadcasted_iota(jnp.int32, (vis, cells), 1).astype(jnp.float32) < count
    for c in range(2):
        seen = observed[pl.ds(c, vis, stride=2), :]
        residual[pl.ds(c, vis, stride=2), :] = jnp.where(mask, seen - gathered(narrow, 0, vis, c), 0.0)
    with scope("given"):
        for copy in given_copies:
            copy.wait()

    @pl.when(has_next)
    def _():
        halo(0, 0, chunks).wait_send()

    @pl.when(has_last)
    def _():
        halo(1, 0, chunks).wait_send()


def dirty_kernel(hot, terms, left, dirty, residual, held, sems):
    blocks, rows, cells = held.shape
    rows = rows // 2
    kept = pltpu.make_async_copy(left, residual, sems.at[blocks])
    kept.start()
    copies = [kept]
    for block in range(blocks):
        out = lax.dot_general(
            hot[block * rows : (block + 1) * rows, :], terms[...], NN, preferred_element_type=jnp.float32
        )
        for c in range(2):
            held[block, pl.ds(c, rows, stride=2), :] = out[:, c * cells : (c + 1) * cells]
        copy = pltpu.make_async_copy(
            held.at[block], dirty.at[pl.ds(block * rows * 2, rows * 2), :], sems.at[block]
        )
        copy.start()
        copies.append(copy)
    for copy in copies:
        copy.wait()


def on_device(sky_model, beam_pattern, kernels, observed, tile_owner, tile_local, vis_count):
    group = lax.axis_size(("bl", "pol"))
    beams = lax.axis_size("beam")
    rows, grid = beam_pattern.shape[1:]
    strip = sky_model.shape[1]
    halo = (grid - strip) // 2
    vis, cells = kernels.shape[1], kernels.shape[3]
    tiles_dev = (grid // 2 // RADIX) * (grid // WIDE) // group
    lanes = 128
    f32, bf16, i32 = jnp.float32, jnp.bfloat16, jnp.int32
    tables, waves = first_tables(grid), second_tables(grid)
    span, period = grid // RADIX, grid // WIDE
    chunks = rows // period
    dma = pltpu.SemaphoreType.DMA
    arrays = (
        sky_model, beam_pattern[0], kernels[0], observed.reshape(vis * 2, cells),
        tile_owner.reshape(1, vis), tile_local, vis_count,
        jnp.asarray(tables), jnp.asarray(waves),
    )

    residual, shared, hot = pl.pallas_call(
        functools.partial(predict_kernel, group, beams, tiles_dev),
        out_shape=(
            pltpu.VMEM((vis * 2, cells), f32),
            pltpu.VMEM((group, vis, 2 * cells), bf16),
            pltpu.VMEM((tiles_dev, group * vis), bf16),
        ),
        in_specs=[HBM] * len(arrays),
        out_specs=(VMEM, VMEM, VMEM),
        scratch_shapes=[
            pltpu.VMEM((rows, strip), bf16),
            pltpu.VMEM((rows, halo), bf16),
            pltpu.VMEM((rows, halo), bf16),
            pltpu.VMEM((rows, grid), bf16),
            pltpu.VMEM((vis, cells, cells), bf16),
            pltpu.VMEM((vis * 2, cells), f32),
            pltpu.VMEM((1, vis), i32),
            pltpu.VMEM((1, vis), i32),
            pltpu.VMEM((1, vis), i32),
            pltpu.SMEM((1, vis), i32),
            pltpu.VMEM(tables.shape, bf16),
            pltpu.VMEM(waves.shape, f32),
            pltpu.VMEM((chunks, 2 * period, 2 * cells), bf16),
            pltpu.VMEM((vis // RADIX, lanes), i32),
            pltpu.VMEM((group, vis // RADIX, lanes), i32),
            pltpu.VMEM((group, vis // RADIX, lanes), i32),
            pltpu.SMEM((group, vis // RADIX, lanes), i32),
            pltpu.VMEM((2, period, span), bf16),
            pltpu.VMEM((RADIX // 2 - 1, period, 2 * span), bf16),
            pltpu.VMEM((2, grid // 2 // RADIX * PITCH, period), f32),
            pltpu.VMEM((group * vis * PITCH, period), f32),
            pltpu.VMEM((group * vis * PITCH, period), f32),
            pltpu.VMEM((group * vis, 2 * cells), f32),
            pltpu.VMEM((group * vis, 2 * cells), bf16),
            pltpu.VMEM((group, vis, 2 * cells), bf16),
            pltpu.VMEM((vis, 2 * cells), bf16),
            pltpu.VMEM((vis * RADIX, cells), f32),
            pltpu.VMEM((vis * RADIX, cells), f32),
            pltpu.VMEM((vis * RADIX, cells), f32),
            pltpu.VMEM((vis * RADIX, cells), f32),
            pltpu.VMEM((vis, cells, cells), bf16),
            dma((len(arrays) + chunks,)),
            dma((2,)), dma((2, chunks)),
            dma((PIECES, group - 1)), dma((1, group - 1)), dma((PIECES, group - 1)), dma((PIECES, group - 1)),
        ],
        compiler_params=pltpu.CompilerParams(
            collective_id=0, has_side_effects=True, vmem_limit_bytes=40 * 1024 * 1024
        ),
        name="predict",
    )(*[pltpu.with_memory_space_constraint(x, pltpu.HBM) for x in arrays])

    blocks = 8
    dirty, residual = pl.pallas_call(
        dirty_kernel,
        out_shape=(
            jax.ShapeDtypeStruct((tiles_dev * 2, cells), f32),
            jax.ShapeDtypeStruct((vis * 2, cells), f32),
        ),
        in_specs=[VMEM, VMEM, VMEM],
        out_specs=(HBM, HBM),
        scratch_shapes=[pltpu.VMEM((blocks, tiles_dev * 2 // blocks, cells), f32), dma((blocks + 1,))],
        compiler_params=pltpu.CompilerParams(vmem_limit_bytes=12 * 1024 * 1024),
        name="dirty",
    )(hot, shared.reshape(group * vis, 2 * cells), residual)
    return (
        residual.reshape(1, vis, 2, cells),
        dirty.reshape(1, tiles_dev, 2, cells),
    )


def solution(mesh):
    placed = (
        P(("tile", "bl", "pol"), "beam"),
        P(("tile", "beam"), ("bl", "pol"), None),
        P(("tile", "beam"), ("bl", "pol"), None, None),
        P(("tile", "beam"), ("bl", "pol"), None, None),
        P(("tile", "beam"), ("bl", "pol"), None),
        P(("tile", "beam"), ("bl", "pol")),
        P(("tile", "beam"), ("bl", "pol")),
    )
    return jax.shard_map(
        on_device,
        mesh=mesh,
        in_specs=placed,
        out_specs=(
            P(("tile", "beam"), ("bl", "pol"), None, None),
            P(("tile", "beam"), ("bl", "pol"), None, None),
        ),
        check_vma=False,
    )
```

```python
import functools
import math

import jax
import jax.numpy as jnp
import numpy as np
from jax import lax
from jax.experimental import pallas as pl
from jax.experimental.pallas import tpu as pltpu
from jax.sharding import PartitionSpec as P

MESH = pl.DeviceIdType.MESH
RADIX = 8
WIDE = 16
PITCH = RADIX + 1
PIECES = 2
scope = jax.named_scope
VMEM = pl.BlockSpec(memory_space=pltpu.VMEM)
HBM = pl.BlockSpec(memory_space=pltpu.HBM)
NT = (((1,), (1,)), ((), ()))
NN = (((1,), (0,)), ((), ()))
TN = (((0,), (0,)), ((), ()))


def wave(rows, cols, period, factor):
    angle = (np.outer(rows, cols) % period) * (2.0 * math.pi / period)
    return np.cos(angle) * factor, np.sin(angle) * factor


def first_tables(grid):
    span = grid // RADIX
    blocks = grid // 2 // RADIX
    cols = np.arange(span)

    def of(i):
        return wave(RADIX * np.arange(blocks) + i, cols, grid, grid**-0.5)

    real = []
    for i in (0, RADIX // 2):
        cos, sin = of(i)
        real.append(np.concatenate([cos, -sin], 0))
    tables = list(real)
    for i in range(1, RADIX // 2):
        tables.extend(of(i))
        tables.extend(of(RADIX - i))
    return np.concatenate(tables, 0).astype(jnp.bfloat16)


def second_tables(grid):
    period = grid // WIDE
    phase = np.stack(wave(np.arange(period), np.arange(period), period, 1.0), 1)
    cos, sin = wave(np.arange(period), np.arange(WIDE), grid, grid**-0.5)
    fine = [np.tile(cos, (1, RADIX)), np.tile(sin, (1, RADIX))]
    cos, sin = wave(np.arange(WIDE), np.arange(WIDE), WIDE, 1.0)
    coarse = np.stack([np.tile(cos, (1, RADIX)), np.tile(sin, (1, RADIX))], 1)
    waves = [phase.reshape(2 * period, -1), *fine, coarse.reshape(2 * WIDE, -1)]
    return np.concatenate(waves, 0).astype(np.float32)


def group_index():
    return lax.axis_index("bl") * lax.axis_size("pol") + lax.axis_index("pol")


class Slots:
    def __init__(self):
        self.chips, self.cores = lax.axis_size("bl"), lax.axis_size("pol")
        self.all = [(turn, core) for turn in range(1, self.chips + 1) for core in range(self.cores)]
        self.own = (self.chips, 0)
        self.peers = [pair for pair in self.all if pair != self.own]

    def number(self, pair):
        return (pair[0] - 1) * self.cores + pair[1]

    def device(self, pair):
        chip = lax.rem(lax.axis_index("bl") + pair[0], self.chips)
        return {"bl": chip, "pol": lax.rem(lax.axis_index("pol") + pair[1], self.cores)}

    def back(self, pair):
        turn = self.chips - pair[0] if pair[0] < self.chips else self.chips
        return turn, (self.cores - pair[1]) % self.cores


def transform_rows(at, pattern, strip, low, high, tables, g_real, g_pair, half):
    span = pattern.shape[1] // RADIX
    width = low.shape[1]
    inner = strip.shape[1]
    step = 32
    root = math.sqrt(0.5)

    def octant(a, src):
        first = a * span
        if first < width:
            return low[src, first : first + span]
        if first < width + inner:
            return strip[src, first - width : first - width + span]
        return high[src, first - width - inner : first - width - inner + span]

    count = g_real.shape[1]

    def fold(index, carry):
        src = pl.ds(pl.multiple_of(at + index * step, step), step)
        parts = [
            (pattern[src, a * span : (a + 1) * span] * octant(a, src)).astype(jnp.float32) for a in range(RADIX)
        ]
        s = [parts[a] + parts[a + 4] for a in range(4)]
        d = [parts[a] - parts[a + 4] for a in range(4)]
        even, odd = s[0] + s[2], s[1] + s[3]
        near, far = root * (d[1] - d[3]), root * (d[1] + d[3])

        def put(ref, lead, first, value):
            ref[lead, pl.ds(pl.multiple_of(first + index * step, step), step), :] = value.astype(jnp.bfloat16)

        put(g_real, 0, 0, even + odd)
        put(g_real, 1, 0, even - odd)
        put(g_pair, 1, 0, s[0] - s[2])
        put(g_pair, 1, count, s[3] - s[1])
        put(g_pair, 0, 0, d[0] + near)
        put(g_pair, 0, count, -(d[2] + far))
        put(g_pair, 2, 0, d[0] - near)
        put(g_pair, 2, count, d[2] - far)
        return carry

    lax.fori_loop(0, count // step, fold, 0, unroll=True)
    blocks = half.shape[1] // PITCH
    re, im = half.at[0], half.at[1]
    for k, i in enumerate((0, RADIX // 2)):
        weights = tables[2 * k * blocks : 2 * (k + 1) * blocks]
        out = lax.dot_general(weights, g_real[k], NT, preferred_element_type=jnp.float32)
        re[pl.ds(i, blocks, stride=PITCH), :] = out[:blocks]
        im[pl.ds(i, blocks, stride=PITCH), :] = out[blocks:]
    for k in (1, 0, 2):
        weights = tables[4 * (1 + k) * blocks : 4 * (2 + k) * blocks]
        out = lax.dot_general(weights, g_pair[k], NT, preferred_element_type=jnp.float32)
        parts = [[out[n * blocks : (n + 1) * blocks, c * count : (c + 1) * count] for c in range(2)] for n in range(4)]
        (cos_re, cos_im), (sin_re, sin_im), (cos_re_m, cos_im_m), (sin_re_m, sin_im_m) = parts
        at, mirror = pl.ds(k + 1, blocks, stride=PITCH), pl.ds(RADIX - 1 - k, blocks, stride=PITCH)
        re[at, :] = cos_re + sin_im
        im[at, :] = cos_im - sin_re
        re[mirror, :] = cos_re_m - sin_im_m
        im[mirror, :] = -sin_re_m - cos_im_m


def turn_tiles(source, sets, codes, waves, half, turned_re, turned_im):
    lanes = codes.shape[2]

    def turn_set(g, carry):
        base = g * RADIX * PITCH
        for n in range(RADIX):
            at = codes[source, sets[0] + g, lanes // 2 + n]
            up = codes[source, sets[0] + g, n]
            cos, sin = waves[pl.ds(at, 1), :], waves[pl.ds(at + 1, 1), :]
            x, y = half[0, pl.ds(up, RADIX), :], half[1, pl.ds(up, RADIX), :]
            rows = pl.ds(base + n, RADIX, stride=PITCH)
            turned_re[rows, :] = x * cos + y * sin
            turned_im[rows, :] = y * cos - x * sin
        return carry

    lax.fori_loop(0, sets[1] - sets[0], turn_set, 0, unroll=True)


def pick_cells(count, weights, turned_re, turned_im):
    def rows_of(ref):
        return jnp.concatenate([ref[n * PITCH : n * PITCH + RADIX, :] for n in range(count * RADIX)], axis=0)

    turned = jnp.concatenate([rows_of(turned_re), rows_of(turned_im)], axis=1).astype(jnp.bfloat16)
    cells_of = lax.dot_general(turned, weights, NN, preferred_element_type=jnp.float32)
    wide = cells_of.shape[1]
    cells_of = cells_of.reshape(count, RADIX, RADIX, wide)
    column = lax.broadcasted_iota(jnp.int32, (RADIX, wide), 1)
    row_of = (column % (wide // 2)) // WIDE
    picked = cells_of[:, 0]
    for i in range(1, RADIX):
        picked = jnp.where((row_of == i)[None], cells_of[:, i], picked)
    return picked.reshape(count * RADIX, wide)


def predict_kernel(
    group, beams, tiles_dev,
    sky, pattern_in, kernels_in, observed_in, owner_in, place_in, counts_in, tables_in, waves_in,
    residual, shared, hot,
    strip, low, high, pattern, kernels, observed, owner, place, counts, counts_s, tables, waves,
    table, code, codes, split, codes_s,
    g_real, g_pair, half, turned_re, turned_im, total, part, came, given, wide, narrow, seen_wide, seen_rows, gram,
    local, halo_send, halo_recv, peer_send, code_recv, part_recv, share_recv,
):
    beam = lax.axis_index("beam")
    me = group_index()
    slots = Slots()
    vis, cells = kernels.shape[0], kernels.shape[1]
    width = low.shape[1]
    period = table.shape[1] // 2
    chunks = pattern.shape[0] // period
    has_next, has_last = beam < beams - 1, beam > 0

    barrier = pltpu.get_barrier_semaphore()

    def greet(device):
        pl.semaphore_signal(barrier, inc=1, device_id=device, device_id_type=MESH)

    @pl.when(has_next)
    def _():
        greet({"beam": beam + 1})

    @pl.when(has_last)
    def _():
        greet({"beam": beam - 1})

    for pair in slots.peers:
        greet(slots.device(pair))

    strips = []
    for n, (first, rows) in enumerate(((0, period), (period, (chunks - 1) * period))):
        if rows:
            at = pl.ds(first, rows)
            strips.append(pltpu.make_async_copy(sky.at[at], strip.at[at], local.at[n]))
            strips[n].start()

    loads = {}
    for n, (name, src, dst) in enumerate((
        ("owner", owner_in, owner), ("place", place_in, place), ("kernels", kernels_in, kernels),
        ("observed", observed_in, observed), ("counts", counts_in, counts), ("counts_s", counts_in, counts_s),
        ("waves", waves_in, waves), ("pattern", pattern_in, pattern), ("tables", tables_in, tables),
    )):
        loads[name] = pltpu.make_async_copy(src, dst, local.at[2 + n])
        loads[name].start()

    strips[0].wait()
    edges = jnp.where(beam < beams - 1, 1, 0) + jnp.where(beam > 0, 1, 0)
    with scope("barrier"):
        pl.semaphore_wait(barrier, group - 1 + edges)

    def halo(side, k, count=1):
        rows = pl.ds(pl.multiple_of(k * period, period), count * period)
        first = 0 if side else strip.shape[1] - width
        return pltpu.make_async_remote_copy(
            src_ref=strip.at[rows, pl.ds(first, width)], dst_ref=(high if side else low).at[rows, :],
            send_sem=halo_send.at[side], recv_sem=halo_recv.at[k],
            device_id={"beam": beam - 1 if side else beam + 1}, device_id_type=MESH,
        )

    def to_peer(pair, source, target, send, recv):
        return pltpu.make_async_remote_copy(
            src_ref=source, dst_ref=target, send_sem=send, recv_sem=recv,
            device_id=slots.device(pair), device_id_type=MESH,
        )

    def wait_for(amount, sem):
        pltpu.make_async_copy(amount, amount, sem).wait()

    early = lax.axis_index("pol") == 0
    for k in range(chunks):
        if k == 1:
            strips[1].wait()

        @pl.when(has_next & early)
        def _():
            halo(0, k).start()

        @pl.when(has_last)
        def _():
            halo(1, k).start()

        @pl.when(has_next & jnp.logical_not(early))
        def _():
            halo(0, k).start()

    loads["owner"].wait()
    loads["place"].wait()
    named = owner[...] * tiles_dev + place[...]
    named = jnp.concatenate([named] * (code.shape[1] // vis), axis=1)
    for g in range(vis // RADIX):
        code[g : g + 1, :] = named if g == 0 else pltpu.roll(named, code.shape[1] - g * RADIX, 1)
    for pair in slots.peers:
        to_peer(pair, code, codes.at[slots.number(pair)], peer_send.at[0], code_recv).start()
    codes[slots.number(slots.own)] = code[...]

    @pl.when(beam == 0)
    def _():
        low[...] = jnp.zeros_like(low)

    @pl.when(beam == beams - 1)
    def _():
        high[...] = jnp.zeros_like(high)

    total[...] = jnp.zeros_like(total)
    wide[...] = jnp.zeros_like(wide)
    seen_wide[...] = jnp.zeros_like(seen_wide)
    for name in ("waves", "kernels", "observed", "counts", "counts_s"):
        loads[name].wait()
    def spread(ref, first, count, c, value):
        rough = value.astype(jnp.bfloat16).astype(jnp.float32)
        ref[pl.ds(first * RADIX + c, count, stride=RADIX), :] = rough
        ref[pl.ds(first * RADIX + 2 + c, count, stride=RADIX), :] = value - rough

    def gathered(ref, first, count, c):
        rows = [ref[pl.ds(first * RADIX + c + d, count, stride=RADIX), :] for d in (0, 2)]
        return rows[0] + rows[1]

    def apply(matrices, dims, first, count):
        def of_tile(r, carry):
            at = pl.ds(pl.multiple_of(r * RADIX, RADIX), RADIX)
            narrow[at, :] = lax.dot_general(
                wide[at, :].astype(jnp.bfloat16), matrices[r], dims, preferred_element_type=jnp.float32
            )
            return carry

        lax.fori_loop(first, first + count, of_tile, 0, unroll=True)

    for k in range(chunks):
        row = 4 * period + 2 * (me * chunks + k)
        cos_c, sin_c = waves[pl.ds(row, 1), :], waves[pl.ds(row + 1, 1), :]
        cos_f, sin_f = waves[2 * period : 3 * period, :], waves[3 * period : 4 * period, :]
        cos = (cos_f * cos_c - sin_f * sin_c).astype(jnp.bfloat16)
        sin = (sin_f * cos_c + cos_f * sin_c).astype(jnp.bfloat16)
        table[k, :period, :cells] = cos
        table[k, :period, cells:] = -sin
        table[k, period:, :cells] = sin
        table[k, period:, cells:] = cos

    for c in range(2):
        spread(seen_wide, 0, vis, c, observed[pl.ds(c, vis, stride=2), :])
    row = lax.broadcasted_iota(jnp.int32, (cells, cells), 0)

    def gram_of(r, carry):
        at = pl.ds(pl.multiple_of(r * RADIX, RADIX), RADIX)
        kernel = kernels[r]
        live = jnp.where(row < counts_s[0, r], kernel.astype(jnp.float32), 0.0).astype(jnp.bfloat16)
        gram[r] = lax.dot_general(kernel, live, TN, preferred_element_type=jnp.float32).astype(jnp.bfloat16)
        seen_rows[at, :] = lax.dot_general(
            seen_wide[at, :].astype(jnp.bfloat16), live, NN, preferred_element_type=jnp.float32
        )
        return carry

    with scope("gram"):
        lax.fori_loop(0, vis, gram_of, 0, unroll=4)
    with scope("codes"):
        wait_for(codes.at[pl.ds(0, group - 1)], code_recv)
        wait_for(codes.at[pl.ds(0, group - 1)], peer_send.at[0])
    lanes = code.shape[1]
    lane = lax.broadcasted_iota(jnp.int32, codes.shape, 2)
    up = lax.shift_right_logical(codes[...], period.bit_length() - 1)
    split[...] = jnp.where(lane < lanes // 2, up * PITCH, (codes[...] & (period - 1)) * 2)
    to_scalar = pltpu.make_async_copy(split, codes_s, local.at[0])
    to_scalar.start()

    fit = lanes // vis
    lane = lax.broadcasted_iota(jnp.int32, (1, lanes), 1)
    keys = []
    for first in range(0, group, fit):
        key = codes[first, 0:1, :]
        for n in range(1, fit):
            key = jnp.where(lane < n * vis, key, codes[first + n, 0:1, :])
        keys.append(key)
    key = jnp.concatenate(keys, axis=1) - me * tiles_dev
    step = 256

    def heat(block, carry):
        at = pl.multiple_of(block * step, step)
        tile = lax.broadcasted_iota(jnp.int32, (step, key.shape[1]), 0)
        hot[pl.ds(at, step), :] = jnp.where(tile == key - at, 1.0, 0.0).astype(jnp.bfloat16)
        return carry

    with scope("heat"):
        lax.fori_loop(0, tiles_dev // step, heat, 0)
    to_scalar.wait()
    for name in ("pattern", "tables"):
        loads[name].wait()

    each = vis // PIECES

    def span_of(pair, piece):
        first = slots.number(pair) * vis + piece * each
        return slice(first, first + each)

    def part_copy(pair, piece):
        target = came.at[slots.number(pair), pl.ds(piece * each, each)]
        return to_peer(pair, part.at[span_of(pair, piece)], target, peer_send.at[1], part_recv.at[piece])

    def of_chunk(k, last):
        with scope("halo"):

            @pl.when(has_last & has_next)
            def _():
                rows = pl.ds(pl.multiple_of(k * period, period), period)
                both = strip.at[rows, pl.ds(0, 2 * width)]
                wait_for(both, halo_recv.at[k])

            @pl.when(has_last & jnp.logical_not(has_next))
            def _():
                halo(0, k).wait_recv()

            @pl.when(has_next & jnp.logical_not(has_last))
            def _():
                halo(1, k).wait_recv()

        with scope("rows"):
            transform_rows(k * period, pattern, strip, low, high, tables, g_real, g_pair, half)
        far = [pair for pair in slots.all if pair[0] < slots.chips]
        near = [pair for pair in slots.all if pair[0] == slots.chips]
        for piece, pair in [(p, q) for some in (far, near) for p in range(PIECES) for q in some]:
            rows = span_of(pair, piece)
            at = slice(rows.start * PITCH, rows.stop * PITCH)
            re, im = turned_re.at[at], turned_im.at[at]
            sets = (piece * each // RADIX, (piece + 1) * each // RADIX)
            turn_tiles(slots.number(slots.back(pair)), sets, codes_s, waves, half, re, im)
            sums = total[rows, :] + pick_cells(each // RADIX, table[k], re, im)
            if last and pair != slots.own:
                part[rows, :] = sums.astype(part.dtype)
                part_copy(pair, piece).start()
            else:
                total[rows, :] = sums

    def chunk_loop(k, carry):
        of_chunk(k, False)
        return carry

    lax.fori_loop(0, chunks - 1, chunk_loop, 0)
    of_chunk(chunks - 1, True)

    for piece in range(PIECES):
        first = piece * each
        mine = total[span_of(slots.own, piece), :]
        with scope("parts"):
            wait_for(came.at[pl.ds(0, group - 1), pl.ds(first, each)], part_recv.at[piece])
        for pair in slots.peers:
            mine = mine + came[slots.number(pair), first : first + each].astype(jnp.float32)
        for c in range(2):
            spread(wide, first, each, c, mine[:, c * cells : (c + 1) * cells])
        with scope("nn"):
            apply(gram, NN, first, each)
        for c in range(2):
            change = gathered(seen_rows, first, each, c) - gathered(narrow, first, each, c)
            given[first : first + each, c * cells : (c + 1) * cells] = change.astype(given.dtype)
        for pair in slots.peers:
            rows = pl.ds(first, each)
            to_peer(pair, given.at[rows], shared.at[slots.number(pair), rows], peer_send.at[2], share_recv).start()
        shared[slots.number(slots.own), first : first + each] = given[first : first + each]

    with scope("nt"):
        apply(kernels, NT, 0, vis)
    eye = lax.broadcasted_iota(jnp.int32, (vis, vis), 0) == lax.broadcasted_iota(jnp.int32, (vis, vis), 1)
    count = jnp.sum(jnp.where(eye, counts[...].astype(jnp.float32), 0.0), axis=1, keepdims=True)
    mask = lax.broadcasted_iota(jnp.int32, (vis, cells), 1).astype(jnp.float32) < count
    for c in range(2):
        seen = observed[pl.ds(c, vis, stride=2), :]
        residual[pl.ds(c, vis, stride=2), :] = jnp.where(mask, seen - gathered(narrow, 0, vis, c), 0.0)
    with scope("given"):
        wait_for(shared.at[pl.ds(0, group - 1)], share_recv)
    wait_for(shared.at[pl.ds(0, group - 1)], peer_send.at[2])
    wait_for(came.at[pl.ds(0, group - 1)], peer_send.at[1])

    @pl.when(has_next)
    def _():
        halo(0, 0, chunks).wait_send()

    @pl.when(has_last)
    def _():
        halo(1, 0, chunks).wait_send()


def dirty_kernel(blocks, hot, terms, left, dirty, residual, held, sems):
    rows = held.shape[0] // blocks
    cells = held.shape[1]
    kept = pltpu.make_async_copy(left, residual, sems.at[1])
    kept.start()
    for block in range(blocks):
        at = pl.ds(block * rows, rows)
        out = lax.dot_general(
            hot[block * rows // 2 : (block + 1) * rows // 2, :], terms[...], NN, preferred_element_type=jnp.float32
        )
        for c in range(2):
            held[pl.ds(block * rows + c, rows // 2, stride=2), :] = out[:, c * cells : (c + 1) * cells]
        pltpu.make_async_copy(held.at[at], dirty.at[at], sems.at[0]).start()
    pltpu.make_async_copy(held, dirty, sems.at[0]).wait()
    kept.wait()


def on_device(sky_model, beam_pattern, kernels, observed, tile_owner, tile_local, vis_count):
    group = lax.axis_size(("bl", "pol"))
    beams = lax.axis_size("beam")
    rows, grid = beam_pattern.shape[1:]
    strip = sky_model.shape[1]
    halo = (grid - strip) // 2
    vis, cells = kernels.shape[1], kernels.shape[3]
    tiles_dev = (grid // 2 // RADIX) * (grid // WIDE) // group
    lanes = 128
    f32, bf16, i32 = jnp.float32, jnp.bfloat16, jnp.int32
    tables, waves = first_tables(grid), second_tables(grid)
    span, period = grid // RADIX, grid // WIDE
    chunks = rows // period
    dma = pltpu.SemaphoreType.DMA
    arrays = (
        sky_model, beam_pattern[0], kernels[0], observed.reshape(vis * 2, cells),
        tile_owner.reshape(1, vis), tile_local, vis_count,
        jnp.asarray(tables), jnp.asarray(waves),
    )

    residual, shared, hot = pl.pallas_call(
        functools.partial(predict_kernel, group, beams, tiles_dev),
        out_shape=(
            pltpu.VMEM((vis * 2, cells), f32),
            pltpu.VMEM((group, vis, 2 * cells), bf16),
            pltpu.VMEM((tiles_dev, group * vis), bf16),
        ),
        in_specs=[HBM] * len(arrays),
        out_specs=(VMEM, VMEM, VMEM),
        scratch_shapes=[
            pltpu.VMEM((rows, strip), bf16),
            pltpu.VMEM((rows, halo), bf16),
            pltpu.VMEM((rows, halo), bf16),
            pltpu.VMEM((rows, grid), bf16),
            pltpu.VMEM((vis, cells, cells), bf16),
            pltpu.VMEM((vis * 2, cells), f32),
            pltpu.VMEM((1, vis), i32),
            pltpu.VMEM((1, vis), i32),
            pltpu.VMEM((1, vis), i32),
            pltpu.SMEM((1, vis), i32),
            pltpu.VMEM(tables.shape, bf16),
            pltpu.VMEM(waves.shape, f32),
            pltpu.VMEM((chunks, 2 * period, 2 * cells), bf16),
            pltpu.VMEM((vis // RADIX, lanes), i32),
            pltpu.VMEM((group, vis // RADIX, lanes), i32),
            pltpu.VMEM((group, vis // RADIX, lanes), i32),
            pltpu.SMEM((group, vis // RADIX, lanes), i32),
            pltpu.VMEM((2, period, span), bf16),
            pltpu.VMEM((RADIX // 2 - 1, 2 * period, span), bf16),
            pltpu.VMEM((2, grid // 2 // RADIX * PITCH, period), f32),
            pltpu.VMEM((group * vis * PITCH, period), f32),
            pltpu.VMEM((group * vis * PITCH, period), f32),
            pltpu.VMEM((group * vis, 2 * cells), f32),
            pltpu.VMEM((group * vis, 2 * cells), bf16),
            pltpu.VMEM((group, vis, 2 * cells), bf16),
            pltpu.VMEM((vis, 2 * cells), bf16),
            pltpu.VMEM((vis * RADIX, cells), f32),
            pltpu.VMEM((vis * RADIX, cells), f32),
            pltpu.VMEM((vis * RADIX, cells), f32),
            pltpu.VMEM((vis * RADIX, cells), f32),
            pltpu.VMEM((vis, cells, cells), bf16),
            dma((len(arrays) + 2,)),
            dma((2,)), dma((chunks,)), dma((3,)), dma, dma((PIECES,)), dma,
        ],
        compiler_params=pltpu.CompilerParams(
            collective_id=0, has_side_effects=True, vmem_limit_bytes=40 * 1024 * 1024
        ),
        name="predict",
    )(*[pltpu.with_memory_space_constraint(x, pltpu.HBM) for x in arrays])

    dirty, residual = pl.pallas_call(
        functools.partial(dirty_kernel, 16),
        out_shape=(
            jax.ShapeDtypeStruct((tiles_dev * 2, cells), f32),
            jax.ShapeDtypeStruct((vis * 2, cells), f32),
        ),
        in_specs=[VMEM, VMEM, VMEM],
        out_specs=(HBM, HBM),
        scratch_shapes=[pltpu.VMEM((tiles_dev * 2, cells), f32), dma((2,))],
        compiler_params=pltpu.CompilerParams(vmem_limit_bytes=12 * 1024 * 1024),
        name="dirty",
    )(hot, shared.reshape(group * vis, 2 * cells), residual)
    return (
        residual.reshape(1, vis, 2, cells),
        dirty.reshape(1, tiles_dev, 2, cells),
    )


def solution(mesh):
    placed = (
        P(("tile", "bl", "pol"), "beam"),
        P(("tile", "beam"), ("bl", "pol"), None),
        P(("tile", "beam"), ("bl", "pol"), None, None),
        P(("tile", "beam"), ("bl", "pol"), None, None),
        P(("tile", "beam"), ("bl", "pol"), None),
        P(("tile", "beam"), ("bl", "pol")),
        P(("tile", "beam"), ("bl", "pol")),
    )
    return jax.shard_map(
        on_device,
        mesh=mesh,
        in_specs=placed,
        out_specs=(
            P(("tile", "beam"), ("bl", "pol"), None, None),
            P(("tile", "beam"), ("bl", "pol"), None, None),
        ),
        check_vma=False,
    )
```

```python
import functools
import math

import jax
import jax.numpy as jnp
import numpy as np
from jax import lax
from jax.experimental import pallas as pl
from jax.experimental.pallas import tpu as pltpu
from jax.sharding import PartitionSpec as P

MESH = pl.DeviceIdType.MESH
RADIX = 8
WIDE = 16
PITCH = RADIX + 1
PIECES = 4
scope = jax.named_scope
VMEM = pl.BlockSpec(memory_space=pltpu.VMEM)
HBM = pl.BlockSpec(memory_space=pltpu.HBM)
NT = (((1,), (1,)), ((), ()))
NN = (((1,), (0,)), ((), ()))
TN = (((0,), (0,)), ((), ()))


def wave(rows, cols, period, factor):
    angle = (np.outer(rows, cols) % period) * (2.0 * math.pi / period)
    return np.cos(angle) * factor, np.sin(angle) * factor


def first_tables(grid):
    span = grid // RADIX
    blocks = grid // 2 // RADIX
    cols = np.arange(span)

    def of(i):
        return wave(RADIX * np.arange(blocks) + i, cols, grid, grid**-0.5)

    real = []
    for i in (0, RADIX // 2):
        cos, sin = of(i)
        real.append(np.concatenate([cos, -sin], 0))
    tables = list(real)
    for i in range(1, RADIX // 2):
        tables.extend(of(i))
        tables.extend(of(RADIX - i))
    return np.concatenate(tables, 0).astype(jnp.bfloat16)


def second_tables(grid):
    period = grid // WIDE
    phase = np.stack(wave(np.arange(period), np.arange(period), period, 1.0), 1)
    cos, sin = wave(np.arange(period), np.arange(WIDE), grid, grid**-0.5)
    fine = [np.tile(cos, (1, RADIX)), np.tile(sin, (1, RADIX))]
    cos, sin = wave(np.arange(WIDE), np.arange(WIDE), WIDE, 1.0)
    coarse = np.stack([np.tile(cos, (1, RADIX)), np.tile(sin, (1, RADIX))], 1)
    waves = [phase.reshape(2 * period, -1), *fine, coarse.reshape(2 * WIDE, -1)]
    return np.concatenate(waves, 0).astype(np.float32)


def group_index():
    return lax.axis_index("bl") * lax.axis_size("pol") + lax.axis_index("pol")


class Slots:
    def __init__(self):
        self.chips, self.cores = lax.axis_size("bl"), lax.axis_size("pol")
        self.all = [(turn, core) for turn in range(1, self.chips + 1) for core in range(self.cores)]
        self.own = (self.chips, 0)
        self.peers = [pair for pair in self.all if pair != self.own]
        self.halves = self.chips == 2 and self.cores == 2

    def number(self, pair):
        return (pair[0] - 1) * self.cores + pair[1]

    def device(self, pair):
        chip = lax.rem(lax.axis_index("bl") + pair[0], self.chips)
        return {"bl": chip, "pol": lax.rem(lax.axis_index("pol") + pair[1], self.cores)}

    def wants(self, pair, piece):
        if not self.halves or pair[0] == self.chips:
            return True
        return (piece < PIECES // 2) == (pair[1] == 0)

    def back(self, pair):
        turn = self.chips - pair[0] if pair[0] < self.chips else self.chips
        return turn, (self.cores - pair[1]) % self.cores


def transform_rows(at, pattern, strip, low, high, tables, g_real, g_pair, half):
    span = pattern.shape[1] // RADIX
    width = low.shape[1]
    inner = strip.shape[1]
    step = 32
    root = math.sqrt(0.5)

    def octant(a, src):
        first = a * span
        if first < width:
            return low[src, first : first + span]
        if first < width + inner:
            return strip[src, first - width : first - width + span]
        return high[src, first - width - inner : first - width - inner + span]

    count = g_real.shape[1]

    def fold(index, carry):
        src = pl.ds(pl.multiple_of(at + index * step, step), step)
        parts = [
            (pattern[src, a * span : (a + 1) * span] * octant(a, src)).astype(jnp.float32) for a in range(RADIX)
        ]
        s = [parts[a] + parts[a + 4] for a in range(4)]
        d = [parts[a] - parts[a + 4] for a in range(4)]
        even, odd = s[0] + s[2], s[1] + s[3]
        near, far = root * (d[1] - d[3]), root * (d[1] + d[3])

        def put(ref, lead, first, value):
            ref[lead, pl.ds(pl.multiple_of(first + index * step, step), step), :] = value.astype(jnp.bfloat16)

        put(g_real, 0, 0, even + odd)
        put(g_real, 1, 0, even - odd)
        put(g_pair, 1, 0, s[0] - s[2])
        put(g_pair, 1, count, s[3] - s[1])
        put(g_pair, 0, 0, d[0] + near)
        put(g_pair, 0, count, -(d[2] + far))
        put(g_pair, 2, 0, d[0] - near)
        put(g_pair, 2, count, d[2] - far)
        return carry

    lax.fori_loop(0, count // step, fold, 0, unroll=True)
    blocks = half.shape[1] // PITCH
    re, im = half.at[0], half.at[1]
    for k, i in enumerate((0, RADIX // 2)):
        weights = tables[2 * k * blocks : 2 * (k + 1) * blocks]
        out = lax.dot_general(weights, g_real[k], NT, preferred_element_type=jnp.float32)
        re[pl.ds(i, blocks, stride=PITCH), :] = out[:blocks]
        im[pl.ds(i, blocks, stride=PITCH), :] = out[blocks:]
    for k in (1, 0, 2):
        weights = tables[4 * (1 + k) * blocks : 4 * (2 + k) * blocks]
        out = lax.dot_general(weights, g_pair[k], NT, preferred_element_type=jnp.float32)
        parts = [[out[n * blocks : (n + 1) * blocks, c * count : (c + 1) * count] for c in range(2)] for n in range(4)]
        (cos_re, cos_im), (sin_re, sin_im), (cos_re_m, cos_im_m), (sin_re_m, sin_im_m) = parts
        at, mirror = pl.ds(k + 1, blocks, stride=PITCH), pl.ds(RADIX - 1 - k, blocks, stride=PITCH)
        re[at, :] = cos_re + sin_im
        im[at, :] = cos_im - sin_re
        re[mirror, :] = cos_re_m - sin_im_m
        im[mirror, :] = -sin_re_m - cos_im_m


def sorted_tiles(owner, place, tiles_dev, firsts):
    vis = owner.shape[1]
    index = lax.broadcasted_iota(jnp.int32, (1, vis), 1)
    none = jnp.zeros((1, vis), jnp.int32)

    def count(r, heads):
        return heads + jnp.where(owner[0, r] == firsts[0], 1, 0)

    def put(r, carry):
        head, tail, middle, named, tile, moved = carry
        name = owner[0, r]
        is_head, is_tail = jnp.where(name == firsts[0], 1, 0), jnp.where(name == firsts[1], 1, 0)
        at = is_head * head + is_tail * tail + (1 - is_head - is_tail) * middle
        here = index == at
        named = jnp.where(here, name * tiles_dev + place[0, r], named)
        tile = jnp.where(here, r, tile)
        moved = jnp.where(index == r, at, moved)
        return head + is_head, tail - is_tail, middle + 1 - is_head - is_tail, named, tile, moved

    heads = lax.fori_loop(0, vis, count, jnp.int32(0), unroll=8)
    return lax.fori_loop(0, vis, put, (jnp.int32(0), jnp.int32(vis - 1), heads, none, none, none), unroll=8)[3:]


def turn_tiles(source, sets, codes, waves, half, turned_re, turned_im):
    lanes = codes.shape[2]

    def turn_set(g, carry):
        base = g * RADIX * PITCH
        for n in range(RADIX):
            at = codes[source, sets[0] + g, lanes // 2 + n]
            up = codes[source, sets[0] + g, n]
            cos, sin = waves[pl.ds(at, 1), :], waves[pl.ds(at + 1, 1), :]
            x, y = half[0, pl.ds(up, RADIX), :], half[1, pl.ds(up, RADIX), :]
            rows = pl.ds(base + n, RADIX, stride=PITCH)
            turned_re[rows, :] = x * cos + y * sin
            turned_im[rows, :] = y * cos - x * sin
        return carry

    lax.fori_loop(0, sets[1] - sets[0], turn_set, 0, unroll=True)


def pick_cells(weights, turned):
    count = sum(re.shape[0] for re, _ in turned) // (RADIX * PITCH)

    def rows_of(n):
        refs = [pair[n] for pair in turned]
        return jnp.concatenate(
            [ref[at : at + RADIX, :] for ref in refs for at in range(0, ref.shape[0], PITCH)], axis=0
        )

    turned = jnp.concatenate([rows_of(0), rows_of(1)], axis=1).astype(jnp.bfloat16)
    cells_of = lax.dot_general(turned, weights, NN, preferred_element_type=jnp.float32)
    wide = cells_of.shape[1]
    cells_of = cells_of.reshape(count, RADIX, RADIX, wide)
    column = lax.broadcasted_iota(jnp.int32, (RADIX, wide), 1)
    row_of = (column % (wide // 2)) // WIDE
    picked = cells_of[:, 0]
    for i in range(1, RADIX):
        picked = jnp.where((row_of == i)[None], cells_of[:, i], picked)
    return picked.reshape(count * RADIX, wide)


def predict_kernel(
    group, beams, tiles_dev,
    sky, pattern_in, kernels_in, observed_in, owner_in, place_in, counts_in, tables_in, waves_in,
    residual, shared, hot,
    strip, low, high, pattern, kernels, observed, owner, place, counts, counts_s, tables, waves,
    table, code, codes, split, codes_s, order, order_s,
    g_real, g_pair, half, turned_re, turned_im, total, part, came, given, wide, narrow, seen_wide, seen_rows, gram,
    local, halo_send, halo_recv, peer_send, code_recv, part_recv, share_recv,
):
    beam = lax.axis_index("beam")
    me = group_index()
    slots = Slots()
    vis, cells = kernels.shape[0], kernels.shape[1]
    width = low.shape[1]
    period = table.shape[1] // 2
    chunks = pattern.shape[0] // period
    has_next, has_last = beam < beams - 1, beam > 0

    barrier = pltpu.get_barrier_semaphore()

    def greet(device):
        pl.semaphore_signal(barrier, inc=1, device_id=device, device_id_type=MESH)

    @pl.when(has_next)
    def _():
        greet({"beam": beam + 1})

    @pl.when(has_last)
    def _():
        greet({"beam": beam - 1})

    for pair in slots.peers:
        greet(slots.device(pair))

    strips = []
    for n, (first, rows) in enumerate(((0, period), (period, (chunks - 1) * period))):
        if rows:
            at = pl.ds(first, rows)
            strips.append(pltpu.make_async_copy(sky.at[at], strip.at[at], local.at[n]))
            strips[n].start()

    loads = {}
    for n, (name, src, dst) in enumerate((
        ("owner", owner_in, owner), ("place", place_in, place), ("kernels", kernels_in, kernels),
        ("observed", observed_in, observed), ("counts", counts_in, counts), ("counts_s", counts_in, counts_s),
        ("waves", waves_in, waves), ("pattern", pattern_in, pattern), ("tables", tables_in, tables),
    )):
        loads[name] = pltpu.make_async_copy(src, dst, local.at[2 + n])
        loads[name].start()

    strips[0].wait()
    edges = jnp.where(beam < beams - 1, 1, 0) + jnp.where(beam > 0, 1, 0)
    with scope("barrier"):
        pl.semaphore_wait(barrier, group - 1 + edges)

    def halo(side, k, count=1):
        rows = pl.ds(pl.multiple_of(k * period, period), count * period)
        first = 0 if side else strip.shape[1] - width
        return pltpu.make_async_remote_copy(
            src_ref=strip.at[rows, pl.ds(first, width)], dst_ref=(high if side else low).at[rows, :],
            send_sem=halo_send.at[side], recv_sem=halo_recv.at[k],
            device_id={"beam": beam - 1 if side else beam + 1}, device_id_type=MESH,
        )

    def to_peer(pair, source, target, send, recv):
        return pltpu.make_async_remote_copy(
            src_ref=source, dst_ref=target, send_sem=send, recv_sem=recv,
            device_id=slots.device(pair), device_id_type=MESH,
        )

    def wait_for(amount, sem):
        pltpu.make_async_copy(amount, amount, sem).wait()

    early = lax.axis_index("pol") == 0
    for k in range(chunks):
        if k == 1:
            strips[1].wait()

        @pl.when(has_next & early)
        def _():
            halo(0, k).start()

        @pl.when(has_last)
        def _():
            halo(1, k).start()

        @pl.when(has_next & jnp.logical_not(early))
        def _():
            halo(0, k).start()

    loads["owner"].wait()
    loads["place"].wait()
    firsts = [slots.device(pair) for pair in slots.all if pair[0] < slots.chips]
    firsts = [first["bl"] * slots.cores + first["pol"] for first in firsts] if slots.halves else [-1, -1]
    named, tile, moved = sorted_tiles(owner, place, tiles_dev, firsts)
    rows = (tile, tile * RADIX, moved * RADIX)
    for n, row in enumerate(rows):
        order[n : n + 1, :] = row
    order_copy = pltpu.make_async_copy(order, order_s, local.at[1])
    order_copy.start()
    named = jnp.concatenate([named] * (code.shape[1] // vis), axis=1)
    for g in range(vis // RADIX):
        code[g : g + 1, :] = named if g == 0 else pltpu.roll(named, code.shape[1] - g * RADIX, 1)
    for pair in slots.peers:
        to_peer(pair, code, codes.at[slots.number(pair)], peer_send.at[0], code_recv).start()
    codes[slots.number(slots.own)] = code[...]

    @pl.when(beam == 0)
    def _():
        low[...] = jnp.zeros_like(low)

    @pl.when(beam == beams - 1)
    def _():
        high[...] = jnp.zeros_like(high)

    order_copy.wait()
    for pair in slots.peers:
        for piece in range(PIECES):
            if not slots.wants(pair, piece):
                each = vis // PIECES
                rows = pl.ds(piece * each, each)
                shared[slots.number(pair), rows] = jnp.zeros((each, shared.shape[2]), shared.dtype)
    total[...] = jnp.zeros_like(total)
    wide[...] = jnp.zeros_like(wide)
    seen_wide[...] = jnp.zeros_like(seen_wide)
    for name in ("waves", "kernels", "observed", "counts", "counts_s"):
        loads[name].wait()
    def spread(ref, first, count, c, value):
        rough = value.astype(jnp.bfloat16).astype(jnp.float32)
        ref[pl.ds(first * RADIX + c, count, stride=RADIX), :] = rough
        ref[pl.ds(first * RADIX + 2 + c, count, stride=RADIX), :] = value - rough

    def gathered(ref, first, count, c):
        rows = [ref[pl.ds(first * RADIX + c + d, count, stride=RADIX), :] for d in (0, 2)]
        return rows[0] + rows[1]

    def rows_at(r):
        return pl.ds(pl.multiple_of(r * RADIX, RADIX), RADIX)

    def change_of(p, carry):
        seen = seen_rows[pl.ds(order_s[1, p], RADIX), :]
        narrow[rows_at(p), :] = seen - lax.dot_general(
            wide[rows_at(p), :].astype(jnp.bfloat16), gram[order_s[0, p]], NN, preferred_element_type=jnp.float32
        )
        return carry

    def predict_of(r, carry):
        narrow[rows_at(r), :] = lax.dot_general(
            wide[pl.ds(order_s[2, r], RADIX), :].astype(jnp.bfloat16), kernels[r], NT, preferred_element_type=jnp.float32
        )
        return carry

    for k in range(chunks):
        row = 4 * period + 2 * (me * chunks + k)
        cos_c, sin_c = waves[pl.ds(row, 1), :], waves[pl.ds(row + 1, 1), :]
        cos_f, sin_f = waves[2 * period : 3 * period, :], waves[3 * period : 4 * period, :]
        cos = (cos_f * cos_c - sin_f * sin_c).astype(jnp.bfloat16)
        sin = (sin_f * cos_c + cos_f * sin_c).astype(jnp.bfloat16)
        table[k, :period, :cells] = cos
        table[k, :period, cells:] = -sin
        table[k, period:, :cells] = sin
        table[k, period:, cells:] = cos

    for c in range(2):
        spread(seen_wide, 0, vis, c, observed[pl.ds(c, vis, stride=2), :])
    row = lax.broadcasted_iota(jnp.int32, (cells, cells), 0)

    def gram_of(r, carry):
        at = pl.ds(pl.multiple_of(r * RADIX, RADIX), RADIX)
        kernel = kernels[r]
        live = jnp.where(row < counts_s[0, r], kernel.astype(jnp.float32), 0.0).astype(jnp.bfloat16)
        gram[r] = lax.dot_general(kernel, live, TN, preferred_element_type=jnp.float32).astype(jnp.bfloat16)
        seen_rows[at, :] = lax.dot_general(
            seen_wide[at, :].astype(jnp.bfloat16), live, NN, preferred_element_type=jnp.float32
        )
        return carry

    with scope("gram"):
        lax.fori_loop(0, vis, gram_of, 0, unroll=4)
    with scope("codes"):
        wait_for(codes.at[pl.ds(0, group - 1)], code_recv)
        wait_for(codes.at[pl.ds(0, group - 1)], peer_send.at[0])
    lanes = code.shape[1]
    lane = lax.broadcasted_iota(jnp.int32, codes.shape, 2)
    up = lax.shift_right_logical(codes[...], period.bit_length() - 1)
    split[...] = jnp.where(lane < lanes // 2, up * PITCH, (codes[...] & (period - 1)) * 2)
    to_scalar = pltpu.make_async_copy(split, codes_s, local.at[0])
    to_scalar.start()

    fit = lanes // vis
    lane = lax.broadcasted_iota(jnp.int32, (1, lanes), 1)
    keys = []
    for first in range(0, group, fit):
        key = codes[first, 0:1, :]
        for n in range(1, fit):
            key = jnp.where(lane < n * vis, key, codes[first + n, 0:1, :])
        keys.append(key)
    key = jnp.concatenate(keys, axis=1) - me * tiles_dev
    step = 256

    def heat(block, carry):
        at = pl.multiple_of(block * step, step)
        tile = lax.broadcasted_iota(jnp.int32, (step, key.shape[1]), 0)
        hot[pl.ds(at, step), :] = jnp.where(tile == key - at, 1.0, 0.0).astype(jnp.bfloat16)
        return carry

    with scope("heat"):
        lax.fori_loop(0, tiles_dev // step, heat, 0)
    to_scalar.wait()
    for name in ("pattern", "tables"):
        loads[name].wait()

    each = vis // PIECES

    def span_of(pair, piece):
        first = slots.number(pair) * vis + piece * each
        return slice(first, first + each)

    def part_copy(pair, piece):
        target = came.at[slots.number(pair), pl.ds(piece * each, each)]
        return to_peer(pair, part.at[span_of(pair, piece)], target, peer_send.at[1], part_recv.at[piece])

    def of_chunk(k, last):
        with scope("halo"):

            @pl.when(has_last & has_next)
            def _():
                rows = pl.ds(pl.multiple_of(k * period, period), period)
                both = strip.at[rows, pl.ds(0, 2 * width)]
                wait_for(both, halo_recv.at[k])

            @pl.when(has_last & jnp.logical_not(has_next))
            def _():
                halo(0, k).wait_recv()

            @pl.when(has_next & jnp.logical_not(has_last))
            def _():
                halo(1, k).wait_recv()

        with scope("rows"):
            transform_rows(k * period, pattern, strip, low, high, tables, g_real, g_pair, half)
        for turn in range(1, slots.chips + 1):
            pairs = [pair for pair in slots.all if pair[0] == turn]
            for piece in range(PIECES):
                sets = (piece * each // RADIX, (piece + 1) * each // RADIX)
                turned = []
                for pair in pairs:
                    rows = span_of(pair, piece)
                    at = slice(rows.start * PITCH, rows.stop * PITCH)
                    turned.append((turned_re.at[at], turned_im.at[at]))
                    turn_tiles(slots.number(slots.back(pair)), sets, codes_s, waves, half, *turned[-1])
                picked = pick_cells(table[k], turned)
                for n, pair in enumerate(pairs):
                    rows = span_of(pair, piece)
                    sums = total[rows, :] + picked[n * each : (n + 1) * each]
                    if last and pair != slots.own:
                        part[rows, :] = sums.astype(part.dtype)
                    else:
                        total[rows, :] = sums
                for pair in pairs:
                    if last and pair != slots.own:
                        part_copy(pair, piece).start()

    def chunk_loop(k, carry):
        of_chunk(k, False)
        return carry

    lax.fori_loop(0, chunks - 1, chunk_loop, 0)
    of_chunk(chunks - 1, True)

    for piece in range(PIECES):
        first = piece * each
        mine = total[span_of(slots.own, piece), :]
        with scope("parts"):
            wait_for(came.at[pl.ds(0, group - 1), pl.ds(first, each)], part_recv.at[piece])
        for pair in slots.peers:
            mine = mine + came[slots.number(pair), first : first + each].astype(jnp.float32)
        for c in range(2):
            spread(wide, first, each, c, mine[:, c * cells : (c + 1) * cells])
        with scope("nn"):
            lax.fori_loop(first, first + each, change_of, 0, unroll=True)
        for c in range(2):
            change = gathered(narrow, first, each, c)
            given[first : first + each, c * cells : (c + 1) * cells] = change.astype(given.dtype)
        for pair in slots.peers:
            rows = pl.ds(first, each)
            if slots.wants(pair, piece):
                to_peer(pair, given.at[rows], shared.at[slots.number(pair), rows], peer_send.at[2], share_recv).start()
        shared[slots.number(slots.own), first : first + each] = given[first : first + each]

    with scope("nt"):
        lax.fori_loop(0, vis, predict_of, 0, unroll=True)
    eye = lax.broadcasted_iota(jnp.int32, (vis, vis), 0) == lax.broadcasted_iota(jnp.int32, (vis, vis), 1)
    count = jnp.sum(jnp.where(eye, counts[...].astype(jnp.float32), 0.0), axis=1, keepdims=True)
    mask = lax.broadcasted_iota(jnp.int32, (vis, cells), 1).astype(jnp.float32) < count
    for c in range(2):
        seen = observed[pl.ds(c, vis, stride=2), :]
        residual[pl.ds(c, vis, stride=2), :] = jnp.where(mask, seen - gathered(narrow, 0, vis, c), 0.0)
    with scope("given"):
        sent = sum(slots.wants(pair, piece) for pair in slots.peers for piece in range(PIECES)) // PIECES
        wait_for(shared.at[pl.ds(0, sent)], share_recv)
    wait_for(shared.at[pl.ds(0, sent)], peer_send.at[2])
    wait_for(came.at[pl.ds(0, group - 1)], peer_send.at[1])

    @pl.when(has_next)
    def _():
        halo(0, 0, chunks).wait_send()

    @pl.when(has_last)
    def _():
        halo(1, 0, chunks).wait_send()


def dirty_kernel(hot, terms, left, dirty, residual, held, sems):
    tiles, terms_of = hot.shape
    cells = held.shape[1]
    kept = pltpu.make_async_copy(left, residual, sems.at[1])
    kept.start()
    first, count = 0, tiles // 64
    while first < tiles:
        out = lax.dot_general(hot[first : first + count, :], terms[...], NN, preferred_element_type=jnp.float32)
        for c in range(2):
            held[pl.ds(2 * first + c, count, stride=2), :] = out[:, c * cells : (c + 1) * cells]
        at = pl.ds(2 * first, 2 * count)
        pltpu.make_async_copy(held.at[at], dirty.at[at], sems.at[0]).start()
        first += count
        count = min(tiles - first, first, tiles // 16)
    pltpu.make_async_copy(held, dirty, sems.at[0]).wait()
    kept.wait()


def on_device(sky_model, beam_pattern, kernels, observed, tile_owner, tile_local, vis_count):
    group = lax.axis_size(("bl", "pol"))
    beams = lax.axis_size("beam")
    rows, grid = beam_pattern.shape[1:]
    strip = sky_model.shape[1]
    halo = (grid - strip) // 2
    vis, cells = kernels.shape[1], kernels.shape[3]
    tiles_dev = (grid // 2 // RADIX) * (grid // WIDE) // group
    lanes = 128
    f32, bf16, i32 = jnp.float32, jnp.bfloat16, jnp.int32
    tables, waves = first_tables(grid), second_tables(grid)
    span, period = grid // RADIX, grid // WIDE
    chunks = rows // period
    dma = pltpu.SemaphoreType.DMA
    arrays = (
        sky_model, beam_pattern[0], kernels[0], observed.reshape(vis * 2, cells),
        tile_owner.reshape(1, vis), tile_local, vis_count,
        jnp.asarray(tables), jnp.asarray(waves),
    )

    residual, shared, hot = pl.pallas_call(
        functools.partial(predict_kernel, group, beams, tiles_dev),
        out_shape=(
            pltpu.VMEM((vis * 2, cells), f32),
            pltpu.VMEM((group, vis, 2 * cells), bf16),
            pltpu.VMEM((tiles_dev, group * vis), bf16),
        ),
        in_specs=[HBM] * len(arrays),
        out_specs=(VMEM, VMEM, VMEM),
        scratch_shapes=[
            pltpu.VMEM((rows, strip), bf16),
            pltpu.VMEM((rows, halo), bf16),
            pltpu.VMEM((rows, halo), bf16),
            pltpu.VMEM((rows, grid), bf16),
            pltpu.VMEM((vis, cells, cells), bf16),
            pltpu.VMEM((vis * 2, cells), f32),
            pltpu.SMEM((1, vis), i32),
            pltpu.SMEM((1, vis), i32),
            pltpu.VMEM((1, vis), i32),
            pltpu.SMEM((1, vis), i32),
            pltpu.VMEM(tables.shape, bf16),
            pltpu.VMEM(waves.shape, f32),
            pltpu.VMEM((chunks, 2 * period, 2 * cells), bf16),
            pltpu.VMEM((vis // RADIX, lanes), i32),
            pltpu.VMEM((group, vis // RADIX, lanes), i32),
            pltpu.VMEM((group, vis // RADIX, lanes), i32),
            pltpu.SMEM((group, vis // RADIX, lanes), i32),
            pltpu.VMEM((3, vis), i32),
            pltpu.SMEM((3, vis), i32),
            pltpu.VMEM((2, period, span), bf16),
            pltpu.VMEM((RADIX // 2 - 1, 2 * period, span), bf16),
            pltpu.VMEM((2, grid // 2 // RADIX * PITCH, period), f32),
            pltpu.VMEM((group * vis * PITCH, period), f32),
            pltpu.VMEM((group * vis * PITCH, period), f32),
            pltpu.VMEM((group * vis, 2 * cells), f32),
            pltpu.VMEM((group * vis, 2 * cells), bf16),
            pltpu.VMEM((group, vis, 2 * cells), bf16),
            pltpu.VMEM((vis, 2 * cells), bf16),
            pltpu.VMEM((vis * RADIX, cells), f32),
            pltpu.VMEM((vis * RADIX, cells), f32),
            pltpu.VMEM((vis * RADIX, cells), f32),
            pltpu.VMEM((vis * RADIX, cells), f32),
            pltpu.VMEM((vis, cells, cells), bf16),
            dma((len(arrays) + 2,)),
            dma((2,)), dma((chunks,)), dma((3,)), dma, dma((PIECES,)), dma,
        ],
        compiler_params=pltpu.CompilerParams(
            collective_id=0, has_side_effects=True, vmem_limit_bytes=40 * 1024 * 1024
        ),
        name="predict",
    )(*[pltpu.with_memory_space_constraint(x, pltpu.HBM) for x in arrays])

    dirty, residual = pl.pallas_call(
        dirty_kernel,
        out_shape=(
            jax.ShapeDtypeStruct((tiles_dev * 2, cells), f32),
            jax.ShapeDtypeStruct((vis * 2, cells), f32),
        ),
        in_specs=[VMEM, VMEM, VMEM],
        out_specs=(HBM, HBM),
        scratch_shapes=[pltpu.VMEM((tiles_dev * 2, cells), f32), dma((2,))],
        compiler_params=pltpu.CompilerParams(vmem_limit_bytes=12 * 1024 * 1024),
        name="dirty",
    )(hot, shared.reshape(group * vis, 2 * cells), residual)
    return (
        residual.reshape(1, vis, 2, cells),
        dirty.reshape(1, tiles_dev, 2, cells),
    )


def solution(mesh):
    placed = (
        P(("tile", "bl", "pol"), "beam"),
        P(("tile", "beam"), ("bl", "pol"), None),
        P(("tile", "beam"), ("bl", "pol"), None, None),
        P(("tile", "beam"), ("bl", "pol"), None, None),
        P(("tile", "beam"), ("bl", "pol"), None),
        P(("tile", "beam"), ("bl", "pol")),
        P(("tile", "beam"), ("bl", "pol")),
    )
    return jax.shard_map(
        on_device,
        mesh=mesh,
        in_specs=placed,
        out_specs=(
            P(("tile", "beam"), ("bl", "pol"), None, None),
            P(("tile", "beam"), ("bl", "pol"), None, None),
        ),
        check_vma=False,
    )
```

```python
import functools
import math

import jax
import jax.numpy as jnp
import numpy as np
from jax import lax
from jax.experimental import pallas as pl
from jax.experimental.pallas import tpu as pltpu
from jax.sharding import PartitionSpec as P

MESH = pl.DeviceIdType.MESH
RADIX = 8
WIDE = 16
PITCH = RADIX + 1
PIECES = 4
scope = jax.named_scope
VMEM = pl.BlockSpec(memory_space=pltpu.VMEM)
HBM = pl.BlockSpec(memory_space=pltpu.HBM)
NT = (((1,), (1,)), ((), ()))
NN = (((1,), (0,)), ((), ()))
TN = (((0,), (0,)), ((), ()))


def wave(rows, cols, period, factor):
    angle = (np.outer(rows, cols) % period) * (2.0 * math.pi / period)
    return np.cos(angle) * factor, np.sin(angle) * factor


def first_tables(grid):
    span = grid // RADIX
    blocks = grid // 2 // RADIX
    cols = np.arange(span)

    def of(i):
        return wave(RADIX * np.arange(blocks) + i, cols, grid, grid**-0.5)

    real = []
    for i in (0, RADIX // 2):
        cos, sin = of(i)
        real.append(np.concatenate([cos, -sin], 0))
    tables = list(real)
    for i in range(1, RADIX // 2):
        tables.extend(of(i))
        tables.extend(of(RADIX - i))
    return np.concatenate(tables, 0).astype(jnp.bfloat16)


def second_tables(grid):
    period = grid // WIDE
    phase = np.stack(wave(np.arange(period), np.arange(period), period, 1.0), 1)
    cos, sin = wave(np.arange(period), np.arange(WIDE), grid, grid**-0.5)
    fine = [np.tile(cos, (1, RADIX)), np.tile(sin, (1, RADIX))]
    cos, sin = wave(np.arange(WIDE), np.arange(WIDE), WIDE, 1.0)
    coarse = np.stack([np.tile(cos, (1, RADIX)), np.tile(sin, (1, RADIX))], 1)
    waves = [phase.reshape(2 * period, -1), *fine, coarse.reshape(2 * WIDE, -1)]
    return np.concatenate(waves, 0).astype(np.float32)


def group_index():
    return lax.axis_index("bl") * lax.axis_size("pol") + lax.axis_index("pol")


class Slots:
    def __init__(self):
        self.chips, self.cores = lax.axis_size("bl"), lax.axis_size("pol")
        self.all = [(turn, core) for turn in range(1, self.chips + 1) for core in range(self.cores)]
        self.own = (self.chips, 0)
        self.peers = [pair for pair in self.all if pair != self.own]
        self.halves = self.chips == 2 and self.cores == 2

    def number(self, pair):
        return (pair[0] - 1) * self.cores + pair[1]

    def device(self, pair):
        chip = lax.rem(lax.axis_index("bl") + pair[0], self.chips)
        return {"bl": chip, "pol": lax.rem(lax.axis_index("pol") + pair[1], self.cores)}

    def wants(self, pair, piece):
        if not self.halves or pair[0] == self.chips:
            return True
        return (piece < PIECES // 2) == (pair[1] == 0)

    def back(self, pair):
        turn = self.chips - pair[0] if pair[0] < self.chips else self.chips
        return turn, (self.cores - pair[1]) % self.cores


def transform_rows(at, pattern, strip, low, high, tables, g_real, g_pair, half):
    span = pattern.shape[1] // RADIX
    width = low.shape[1]
    inner = strip.shape[1]
    step = 32
    root = math.sqrt(0.5)

    def octant(a, src):
        first = a * span
        if first < width:
            return low[src, first : first + span]
        if first < width + inner:
            return strip[src, first - width : first - width + span]
        return high[src, first - width - inner : first - width - inner + span]

    count = g_real.shape[1]

    def fold(index, carry):
        src = pl.ds(pl.multiple_of(at + index * step, step), step)
        parts = [
            (pattern[src, a * span : (a + 1) * span] * octant(a, src)).astype(jnp.float32) for a in range(RADIX)
        ]
        s = [parts[a] + parts[a + 4] for a in range(4)]
        d = [parts[a] - parts[a + 4] for a in range(4)]
        even, odd = s[0] + s[2], s[1] + s[3]
        near, far = root * (d[1] - d[3]), root * (d[1] + d[3])

        def put(ref, lead, first, value):
            ref[lead, pl.ds(pl.multiple_of(first + index * step, step), step), :] = value.astype(jnp.bfloat16)

        put(g_real, 0, 0, even + odd)
        put(g_real, 1, 0, even - odd)
        put(g_pair, 1, 0, s[0] - s[2])
        put(g_pair, 1, count, s[3] - s[1])
        put(g_pair, 0, 0, d[0] + near)
        put(g_pair, 0, count, -(d[2] + far))
        put(g_pair, 2, 0, d[0] - near)
        put(g_pair, 2, count, d[2] - far)
        return carry

    lax.fori_loop(0, count // step, fold, 0, unroll=True)
    blocks = half.shape[1] // PITCH
    re, im = half.at[0], half.at[1]
    for k, i in enumerate((0, RADIX // 2)):
        weights = tables[2 * k * blocks : 2 * (k + 1) * blocks]
        out = lax.dot_general(weights, g_real[k], NT, preferred_element_type=jnp.float32)
        re[pl.ds(i, blocks, stride=PITCH), :] = out[:blocks]
        im[pl.ds(i, blocks, stride=PITCH), :] = out[blocks:]
    for k in (1, 0, 2):
        weights = tables[4 * (1 + k) * blocks : 4 * (2 + k) * blocks]
        out = lax.dot_general(weights, g_pair[k], NT, preferred_element_type=jnp.float32)
        parts = [[out[n * blocks : (n + 1) * blocks, c * count : (c + 1) * count] for c in range(2)] for n in range(4)]
        (cos_re, cos_im), (sin_re, sin_im), (cos_re_m, cos_im_m), (sin_re_m, sin_im_m) = parts
        at, mirror = pl.ds(k + 1, blocks, stride=PITCH), pl.ds(RADIX - 1 - k, blocks, stride=PITCH)
        re[at, :] = cos_re + sin_im
        im[at, :] = cos_im - sin_re
        re[mirror, :] = cos_re_m - sin_im_m
        im[mirror, :] = -sin_re_m - cos_im_m


def sorted_tiles(owner, place, tiles_dev, firsts):
    vis = owner.shape[1]
    index = lax.broadcasted_iota(jnp.int32, (1, vis), 1)
    none = jnp.zeros((1, vis), jnp.int32)

    def count(r, heads):
        return heads + jnp.where(owner[0, r] == firsts[0], 1, 0)

    def put(r, carry):
        head, tail, middle, named, tile, moved = carry
        name = owner[0, r]
        is_head, is_tail = jnp.where(name == firsts[0], 1, 0), jnp.where(name == firsts[1], 1, 0)
        at = is_head * head + is_tail * tail + (1 - is_head - is_tail) * middle
        here = index == at
        named = jnp.where(here, name * tiles_dev + place[0, r], named)
        tile = jnp.where(here, r, tile)
        moved = jnp.where(index == r, at, moved)
        return head + is_head, tail - is_tail, middle + 1 - is_head - is_tail, named, tile, moved

    heads = lax.fori_loop(0, vis, count, jnp.int32(0), unroll=8)
    return lax.fori_loop(0, vis, put, (jnp.int32(0), jnp.int32(vis - 1), heads, none, none, none), unroll=8)[3:]


def turn_tiles(source, sets, codes, waves, half, turned_re, turned_im):
    lanes = codes.shape[2]

    def turn_set(g, carry):
        base = g * RADIX * PITCH
        for n in range(RADIX):
            at = codes[source, sets[0] + g, lanes // 2 + n]
            up = codes[source, sets[0] + g, n]
            cos, sin = waves[pl.ds(at, 1), :], waves[pl.ds(at + 1, 1), :]
            x, y = half[0, pl.ds(up, RADIX), :], half[1, pl.ds(up, RADIX), :]
            rows = pl.ds(base + n, RADIX, stride=PITCH)
            turned_re[rows, :] = x * cos + y * sin
            turned_im[rows, :] = y * cos - x * sin
        return carry

    lax.fori_loop(0, sets[1] - sets[0], turn_set, 0, unroll=True)


def pick_cells(weights, turned):
    count = sum(re.shape[0] for re, _ in turned) // (RADIX * PITCH)

    def rows_of(n):
        refs = [pair[n] for pair in turned]
        return jnp.concatenate(
            [ref[at : at + RADIX, :] for ref in refs for at in range(0, ref.shape[0], PITCH)], axis=0
        )

    turned = jnp.concatenate([rows_of(0), rows_of(1)], axis=1).astype(jnp.bfloat16)
    cells_of = lax.dot_general(turned, weights, NN, preferred_element_type=jnp.float32)
    wide = cells_of.shape[1]
    cells_of = cells_of.reshape(count, RADIX, RADIX, wide)
    column = lax.broadcasted_iota(jnp.int32, (RADIX, wide), 1)
    row_of = (column % (wide // 2)) // WIDE
    picked = cells_of[:, 0]
    for i in range(1, RADIX):
        picked = jnp.where((row_of == i)[None], cells_of[:, i], picked)
    return picked.reshape(count * RADIX, wide)


def predict_kernel(
    group, beams, tiles_dev,
    sky, pattern_in, kernels_in, observed_in, owner_in, place_in, counts_in, tables_in, waves_in,
    residual, shared, hot,
    strip, low, high, pattern, kernels, observed, owner, place, counts, counts_s, tables, waves,
    table, code, codes, split, codes_s, order, order_s,
    g_real, g_pair, half, turned_re, turned_im, total, part, came, given, wide, narrow, seen_wide, seen_rows, gram,
    local, halo_send, halo_recv, peer_send, code_recv, part_recv, share_recv,
):
    beam = lax.axis_index("beam")
    me = group_index()
    slots = Slots()
    vis, cells = kernels.shape[0], kernels.shape[1]
    width = low.shape[1]
    period = table.shape[1] // 2
    chunks = pattern.shape[0] // period
    has_next, has_last = beam < beams - 1, beam > 0

    barrier = pltpu.get_barrier_semaphore()

    def greet(device):
        pl.semaphore_signal(barrier, inc=1, device_id=device, device_id_type=MESH)

    @pl.when(has_next)
    def _():
        greet({"beam": beam + 1})

    @pl.when(has_last)
    def _():
        greet({"beam": beam - 1})

    for pair in slots.peers:
        greet(slots.device(pair))

    strips = []
    for n, (first, rows) in enumerate(((0, period), (period, (chunks - 1) * period))):
        if rows:
            at = pl.ds(first, rows)
            strips.append(pltpu.make_async_copy(sky.at[at], strip.at[at], local.at[n]))
            strips[n].start()

    loads = {}
    for n, (name, src, dst) in enumerate((
        ("owner", owner_in, owner), ("place", place_in, place), ("kernels", kernels_in, kernels),
        ("observed", observed_in, observed), ("counts", counts_in, counts), ("counts_s", counts_in, counts_s),
        ("waves", waves_in, waves), ("pattern", pattern_in, pattern), ("tables", tables_in, tables),
    )):
        loads[name] = pltpu.make_async_copy(src, dst, local.at[2 + n])
        loads[name].start()

    strips[0].wait()
    edges = jnp.where(beam < beams - 1, 1, 0) + jnp.where(beam > 0, 1, 0)
    with scope("barrier"):
        pl.semaphore_wait(barrier, group - 1 + edges)

    def halo(side, k, count=1):
        rows = pl.ds(pl.multiple_of(k * period, period), count * period)
        first = 0 if side else strip.shape[1] - width
        return pltpu.make_async_remote_copy(
            src_ref=strip.at[rows, pl.ds(first, width)], dst_ref=(high if side else low).at[rows, :],
            send_sem=halo_send.at[side], recv_sem=halo_recv.at[k],
            device_id={"beam": beam - 1 if side else beam + 1}, device_id_type=MESH,
        )

    def to_peer(pair, source, target, send, recv):
        return pltpu.make_async_remote_copy(
            src_ref=source, dst_ref=target, send_sem=send, recv_sem=recv,
            device_id=slots.device(pair), device_id_type=MESH,
        )

    def wait_for(amount, sem):
        pltpu.make_async_copy(amount, amount, sem).wait()

    early = lax.axis_index("pol") == 0
    for k in range(chunks):
        if k == 1:
            strips[1].wait()

        @pl.when(has_next & early)
        def _():
            halo(0, k).start()

        @pl.when(has_last)
        def _():
            halo(1, k).start()

        @pl.when(has_next & jnp.logical_not(early))
        def _():
            halo(0, k).start()

    loads["owner"].wait()
    loads["place"].wait()
    firsts = [slots.device(pair) for pair in slots.all if pair[0] < slots.chips]
    firsts = [first["bl"] * slots.cores + first["pol"] for first in firsts] if slots.halves else [-1, -1]
    named, tile, moved = sorted_tiles(owner, place, tiles_dev, firsts)
    rows = (tile, tile * RADIX, moved * RADIX)
    for n, row in enumerate(rows):
        order[n : n + 1, :] = row
    order_copy = pltpu.make_async_copy(order, order_s, local.at[1])
    order_copy.start()
    named = jnp.concatenate([named] * (code.shape[1] // vis), axis=1)
    for g in range(vis // RADIX):
        code[g : g + 1, :] = named if g == 0 else pltpu.roll(named, code.shape[1] - g * RADIX, 1)
    for pair in slots.peers:
        to_peer(pair, code, codes.at[slots.number(pair)], peer_send.at[0], code_recv).start()
    codes[slots.number(slots.own)] = code[...]

    @pl.when(beam == 0)
    def _():
        low[...] = jnp.zeros_like(low)

    @pl.when(beam == beams - 1)
    def _():
        high[...] = jnp.zeros_like(high)

    order_copy.wait()
    for pair in slots.peers:
        for piece in range(PIECES):
            if not slots.wants(pair, piece):
                each = vis // PIECES
                rows = pl.ds(piece * each, each)
                shared[slots.number(pair), rows] = jnp.zeros((each, shared.shape[2]), shared.dtype)
    total[...] = jnp.zeros_like(total)
    wide[...] = jnp.zeros_like(wide)
    seen_wide[...] = jnp.zeros_like(seen_wide)
    for name in ("waves", "kernels", "observed", "counts", "counts_s"):
        loads[name].wait()
    def spread(ref, first, count, c, value):
        rough = value.astype(jnp.bfloat16).astype(jnp.float32)
        ref[pl.ds(first * RADIX + c, count, stride=RADIX), :] = rough
        ref[pl.ds(first * RADIX + 2 + c, count, stride=RADIX), :] = value - rough

    def gathered(ref, first, count, c):
        rows = [ref[pl.ds(first * RADIX + c + d, count, stride=RADIX), :] for d in (0, 2)]
        return rows[0] + rows[1]

    def rows_at(r):
        return pl.ds(pl.multiple_of(r * RADIX, RADIX), RADIX)

    def change_of(p, carry):
        seen = seen_rows[pl.ds(order_s[1, p], RADIX), :]
        narrow[rows_at(p), :] = seen - lax.dot_general(
            wide[rows_at(p), :].astype(jnp.bfloat16), gram[order_s[0, p]], NN, preferred_element_type=jnp.float32
        )
        return carry

    def predict_of(r, carry):
        narrow[rows_at(r), :] = lax.dot_general(
            wide[pl.ds(order_s[2, r], RADIX), :].astype(jnp.bfloat16), kernels[r], NT, preferred_element_type=jnp.float32
        )
        return carry

    for k in range(chunks):
        row = 4 * period + 2 * (me * chunks + k)
        cos_c, sin_c = waves[pl.ds(row, 1), :], waves[pl.ds(row + 1, 1), :]
        cos_f, sin_f = waves[2 * period : 3 * period, :], waves[3 * period : 4 * period, :]
        cos = (cos_f * cos_c - sin_f * sin_c).astype(jnp.bfloat16)
        sin = (sin_f * cos_c + cos_f * sin_c).astype(jnp.bfloat16)
        table[k, :period, :cells] = cos
        table[k, :period, cells:] = -sin
        table[k, period:, :cells] = sin
        table[k, period:, cells:] = cos

    for c in range(2):
        spread(seen_wide, 0, vis, c, observed[pl.ds(c, vis, stride=2), :])
    row = lax.broadcasted_iota(jnp.int32, (cells, cells), 0)

    def gram_of(r, carry):
        at = pl.ds(pl.multiple_of(r * RADIX, RADIX), RADIX)
        kernel = kernels[r]
        live = jnp.where(row < counts_s[0, r], kernel.astype(jnp.float32), 0.0).astype(jnp.bfloat16)
        gram[r] = lax.dot_general(kernel, live, TN, preferred_element_type=jnp.float32).astype(jnp.bfloat16)
        seen_rows[at, :] = lax.dot_general(
            seen_wide[at, :].astype(jnp.bfloat16), live, NN, preferred_element_type=jnp.float32
        )
        return carry

    with scope("gram"):
        lax.fori_loop(0, vis, gram_of, 0, unroll=4)
    with scope("codes"):
        wait_for(codes.at[pl.ds(0, group - 1)], code_recv)
        wait_for(codes.at[pl.ds(0, group - 1)], peer_send.at[0])
    lanes = code.shape[1]
    lane = lax.broadcasted_iota(jnp.int32, codes.shape, 2)
    up = lax.shift_right_logical(codes[...], period.bit_length() - 1)
    split[...] = jnp.where(lane < lanes // 2, up * PITCH, (codes[...] & (period - 1)) * 2)
    to_scalar = pltpu.make_async_copy(split, codes_s, local.at[0])
    to_scalar.start()

    fit = lanes // vis
    lane = lax.broadcasted_iota(jnp.int32, (1, lanes), 1)
    keys = []
    for first in range(0, group, fit):
        key = codes[first, 0:1, :]
        for n in range(1, fit):
            key = jnp.where(lane < n * vis, key, codes[first + n, 0:1, :])
        keys.append(key)
    key = jnp.concatenate(keys, axis=1) - me * tiles_dev
    step = 256

    def heat(block, carry):
        at = pl.multiple_of(block * step, step)
        tile = lax.broadcasted_iota(jnp.int32, (step, key.shape[1]), 0)
        hot[pl.ds(at, step), :] = jnp.where(tile == key - at, 1.0, 0.0).astype(jnp.bfloat16)
        return carry

    with scope("heat"):
        lax.fori_loop(0, tiles_dev // step, heat, 0)
    to_scalar.wait()
    for name in ("pattern", "tables"):
        loads[name].wait()

    each = vis // PIECES

    def span_of(pair, piece):
        first = slots.number(pair) * vis + piece * each
        return slice(first, first + each)

    def part_copy(pair, piece):
        target = came.at[slots.number(pair), pl.ds(piece * each, each)]
        return to_peer(pair, part.at[span_of(pair, piece)], target, peer_send.at[1], part_recv.at[piece])

    def of_chunk(k, last):
        with scope("halo"):

            @pl.when(has_last & has_next)
            def _():
                rows = pl.ds(pl.multiple_of(k * period, period), period)
                both = strip.at[rows, pl.ds(0, 2 * width)]
                wait_for(both, halo_recv.at[k])

            @pl.when(has_last & jnp.logical_not(has_next))
            def _():
                halo(0, k).wait_recv()

            @pl.when(has_next & jnp.logical_not(has_last))
            def _():
                halo(1, k).wait_recv()

        with scope("rows"):
            transform_rows(k * period, pattern, strip, low, high, tables, g_real, g_pair, half)
        for turn in range(1, slots.chips + 1):
            pairs = [pair for pair in slots.all if pair[0] == turn]
            for piece in range(PIECES):
                sets = (piece * each // RADIX, (piece + 1) * each // RADIX)
                turned = []
                for pair in pairs:
                    rows = span_of(pair, piece)
                    at = slice(rows.start * PITCH, rows.stop * PITCH)
                    turned.append((turned_re.at[at], turned_im.at[at]))
                    turn_tiles(slots.number(slots.back(pair)), sets, codes_s, waves, half, *turned[-1])
                picked = pick_cells(table[k], turned)
                for n, pair in enumerate(pairs):
                    rows = span_of(pair, piece)
                    sums = total[rows, :] + picked[n * each : (n + 1) * each]
                    if last and pair != slots.own:
                        part[rows, :] = sums.astype(part.dtype)
                    else:
                        total[rows, :] = sums
                for pair in pairs:
                    if last and pair != slots.own:
                        part_copy(pair, piece).start()

    def chunk_loop(k, carry):
        of_chunk(k, False)
        return carry

    lax.fori_loop(0, chunks - 1, chunk_loop, 0)
    of_chunk(chunks - 1, True)

    for piece in range(PIECES):
        first = piece * each
        mine = total[span_of(slots.own, piece), :]
        with scope("parts"):
            wait_for(came.at[pl.ds(0, group - 1), pl.ds(first, each)], part_recv.at[piece])
        for pair in slots.peers:
            mine = mine + came[slots.number(pair), first : first + each].astype(jnp.float32)
        for c in range(2):
            spread(wide, first, each, c, mine[:, c * cells : (c + 1) * cells])
        with scope("nn"):
            lax.fori_loop(first, first + each, change_of, 0, unroll=True)
        for c in range(2):
            change = gathered(narrow, first, each, c)
            given[first : first + each, c * cells : (c + 1) * cells] = change.astype(given.dtype)
        for pair in slots.peers:
            rows = pl.ds(first, each)
            if slots.wants(pair, piece):
                to_peer(pair, given.at[rows], shared.at[slots.number(pair), rows], peer_send.at[2], share_recv).start()
        shared[slots.number(slots.own), first : first + each] = given[first : first + each]

    with scope("nt"):
        lax.fori_loop(0, vis, predict_of, 0, unroll=True)
    eye = lax.broadcasted_iota(jnp.int32, (vis, vis), 0) == lax.broadcasted_iota(jnp.int32, (vis, vis), 1)
    count = jnp.sum(jnp.where(eye, counts[...].astype(jnp.float32), 0.0), axis=1, keepdims=True)
    mask = lax.broadcasted_iota(jnp.int32, (vis, cells), 1).astype(jnp.float32) < count
    for c in range(2):
        seen = observed[pl.ds(c, vis, stride=2), :]
        residual[pl.ds(c, vis, stride=2), :] = jnp.where(mask, seen - gathered(narrow, 0, vis, c), 0.0)
    with scope("given"):
        sent = sum(slots.wants(pair, piece) for pair in slots.peers for piece in range(PIECES)) // PIECES
        wait_for(shared.at[pl.ds(0, sent)], share_recv)
    wait_for(shared.at[pl.ds(0, sent)], peer_send.at[2])
    wait_for(came.at[pl.ds(0, group - 1)], peer_send.at[1])

    @pl.when(has_next)
    def _():
        halo(0, 0, chunks).wait_send()

    @pl.when(has_last)
    def _():
        halo(1, 0, chunks).wait_send()


def dirty_kernel(hot, terms, left, dirty, residual, held, sems):
    tiles, terms_of = hot.shape
    cells = held.shape[1]
    kept = pltpu.make_async_copy(left, residual, sems.at[1])
    kept.start()
    first, count = 0, tiles // 32
    while first < tiles:
        out = lax.dot_general(hot[first : first + count, :], terms[...], NN, preferred_element_type=jnp.float32)
        for c in range(2):
            held[pl.ds(2 * first + c, count, stride=2), :] = out[:, c * cells : (c + 1) * cells]
        at = pl.ds(2 * first, 2 * count)
        pltpu.make_async_copy(held.at[at], dirty.at[at], sems.at[0]).start()
        first += count
        count = min(tiles - first, first, tiles // 32)
    pltpu.make_async_copy(held, dirty, sems.at[0]).wait()
    kept.wait()


def on_device(sky_model, beam_pattern, kernels, observed, tile_owner, tile_local, vis_count):
    group = lax.axis_size(("bl", "pol"))
    beams = lax.axis_size("beam")
    rows, grid = beam_pattern.shape[1:]
    strip = sky_model.shape[1]
    halo = (grid - strip) // 2
    vis, cells = kernels.shape[1], kernels.shape[3]
    tiles_dev = (grid // 2 // RADIX) * (grid // WIDE) // group
    lanes = 128
    f32, bf16, i32 = jnp.float32, jnp.bfloat16, jnp.int32
    tables, waves = first_tables(grid), second_tables(grid)
    span, period = grid // RADIX, grid // WIDE
    chunks = rows // period
    dma = pltpu.SemaphoreType.DMA
    arrays = (
        sky_model, beam_pattern[0], kernels[0], observed.reshape(vis * 2, cells),
        tile_owner.reshape(1, vis), tile_local, vis_count,
        jnp.asarray(tables), jnp.asarray(waves),
    )

    residual, shared, hot = pl.pallas_call(
        functools.partial(predict_kernel, group, beams, tiles_dev),
        out_shape=(
            pltpu.VMEM((vis * 2, cells), f32),
            pltpu.VMEM((group, vis, 2 * cells), bf16),
            pltpu.VMEM((tiles_dev, group * vis), bf16),
        ),
        in_specs=[HBM] * len(arrays),
        out_specs=(VMEM, VMEM, VMEM),
        scratch_shapes=[
            pltpu.VMEM((rows, strip), bf16),
            pltpu.VMEM((rows, halo), bf16),
            pltpu.VMEM((rows, halo), bf16),
            pltpu.VMEM((rows, grid), bf16),
            pltpu.VMEM((vis, cells, cells), bf16),
            pltpu.VMEM((vis * 2, cells), f32),
            pltpu.SMEM((1, vis), i32),
            pltpu.SMEM((1, vis), i32),
            pltpu.VMEM((1, vis), i32),
            pltpu.SMEM((1, vis), i32),
            pltpu.VMEM(tables.shape, bf16),
            pltpu.VMEM(waves.shape, f32),
            pltpu.VMEM((chunks, 2 * period, 2 * cells), bf16),
            pltpu.VMEM((vis // RADIX, lanes), i32),
            pltpu.VMEM((group, vis // RADIX, lanes), i32),
            pltpu.VMEM((group, vis // RADIX, lanes), i32),
            pltpu.SMEM((group, vis // RADIX, lanes), i32),
            pltpu.VMEM((3, vis), i32),
            pltpu.SMEM((3, vis), i32),
            pltpu.VMEM((2, period, span), bf16),
            pltpu.VMEM((RADIX // 2 - 1, 2 * period, span), bf16),
            pltpu.VMEM((2, grid // 2 // RADIX * PITCH, period), f32),
            pltpu.VMEM((group * vis * PITCH, period), f32),
            pltpu.VMEM((group * vis * PITCH, period), f32),
            pltpu.VMEM((group * vis, 2 * cells), f32),
            pltpu.VMEM((group * vis, 2 * cells), bf16),
            pltpu.VMEM((group, vis, 2 * cells), bf16),
            pltpu.VMEM((vis, 2 * cells), bf16),
            pltpu.VMEM((vis * RADIX, cells), f32),
            pltpu.VMEM((vis * RADIX, cells), f32),
            pltpu.VMEM((vis * RADIX, cells), f32),
            pltpu.VMEM((vis * RADIX, cells), f32),
            pltpu.VMEM((vis, cells, cells), bf16),
            dma((len(arrays) + 2,)),
            dma((2,)), dma((chunks,)), dma((3,)), dma, dma((PIECES,)), dma,
        ],
        compiler_params=pltpu.CompilerParams(
            collective_id=0, has_side_effects=True, vmem_limit_bytes=40 * 1024 * 1024
        ),
        name="predict",
    )(*[pltpu.with_memory_space_constraint(x, pltpu.HBM) for x in arrays])

    dirty, residual = pl.pallas_call(
        dirty_kernel,
        out_shape=(
            jax.ShapeDtypeStruct((tiles_dev * 2, cells), f32),
            jax.ShapeDtypeStruct((vis * 2, cells), f32),
        ),
        in_specs=[VMEM, VMEM, VMEM],
        out_specs=(HBM, HBM),
        scratch_shapes=[pltpu.VMEM((tiles_dev * 2, cells), f32), dma((2,))],
        compiler_params=pltpu.CompilerParams(vmem_limit_bytes=12 * 1024 * 1024),
        name="dirty",
    )(hot, shared.reshape(group * vis, 2 * cells), residual)
    return (
        residual.reshape(1, vis, 2, cells),
        dirty.reshape(1, tiles_dev, 2, cells),
    )


def solution(mesh):
    placed = (
        P(("tile", "bl", "pol"), "beam"),
        P(("tile", "beam"), ("bl", "pol"), None),
        P(("tile", "beam"), ("bl", "pol"), None, None),
        P(("tile", "beam"), ("bl", "pol"), None, None),
        P(("tile", "beam"), ("bl", "pol"), None),
        P(("tile", "beam"), ("bl", "pol")),
        P(("tile", "beam"), ("bl", "pol")),
    )
    return jax.shard_map(
        on_device,
        mesh=mesh,
        in_specs=placed,
        out_specs=(
            P(("tile", "beam"), ("bl", "pol"), None, None),
            P(("tile", "beam"), ("bl", "pol"), None, None),
        ),
        check_vma=False,
    )
```
